128 devices in a mesh: tau: 8 (over x, core), tile: 16 (over z, y).
Axes of the slice: x: 4, y: 4, z: 4, core: 2. Of those that a mesh axis runs over, the one named last changes fastest.
Arguments:
- occupied: bfloat16 [8, 2048, 128, 128], P('tau', 'tile'), may hold values from -6 to 6
- virtual: bfloat16 [8, 2048, 128, 128], P('tau', 'tile'), may hold values from -0.125 to 0.125
- cos_weights: float32 [4, 8], replicated, may hold values from -1 to 1
- pair_occ: int32 [3072, 16], P('tile'), may hold values from 0 to 127
- pair_virt: int32 [3072, 16], P('tile'), may hold values from 0 to 127
- partial_target_tile: int32 [3072], P('tile'), may hold values from 0 to 511, as said below
Outputs:
- spectrum: float32 [4, 512, 128, 128], P(None, 'tile', 'tau')
The draws below stay inside these ranges and needn't reach their ends.
Inputs may be any that keep to these rules, and one draw needn't show every extreme that they name: `partial_target_tile`: within each aligned block of 192 entries, no owner (values d * 32 to (d + 1) * 32 - 1 for owner d) is named more than 24 times; one owner is named exactly 24 times in every block.
All inputs are finite; a program needn't handle non-finite values.
Results may differ from the reference program's by a relative error of at most 0.0003.
Values sent between devices are 32-bit elements; how exact they have to be, the bound alone decides.
No kernel may reach another device: no remote copies, remote signals or barrier semaphores. Data moves between devices by JAX's collectives and lax.ppermute only.
A program may use at most 192 MiB of HBM per device.

```python
import math
import jax
import jax.numpy as jnp
from jax import lax

TILE = 128
TERMS = 16
NFREQ = 4
SLOT_DEV = 128
PART_DEV = 192
CHI_DEV = 32
NTAU = 8
NOCC = 2048
NPART = 3072
NCHI = 512
CAP = 24


def draw_partial_target_tile(key, part):
    owners = NPART // PART_DEV
    first, second, third, fourth = jax.random.split(jax.random.fold_in(key, 7), 4)
    complete_holder = jax.random.randint(first, (), 0, owners)
    owner_preference = jax.random.randint(second, (owners, owners), 0, 1 << 19)
    random_perturbation = jax.random.randint(third, (owners, owners, CAP), 0, 1 << 19)
    holder_indices = jnp.arange(owners, dtype=jnp.int32)
    extra_credit = jnp.where(holder_indices == complete_holder, 1 << 20, 0).astype(jnp.int32)
    ranking_value = owner_preference[:, :, None] + random_perturbation + extra_credit[None, :, None]
    places = jnp.arange(owners * CAP, dtype=jnp.int32).reshape(owners, CAP)
    ranking_value = ranking_value * (owners * CAP) + places[None]
    flat = ranking_value.reshape(owners, owners * CAP)
    _, chosen = lax.top_k(flat, PART_DEV)
    owner = (chosen // CAP).astype(jnp.int32)
    within = jax.random.randint(fourth, (owners, PART_DEV), 0, CHI_DEV)
    return (owner * CHI_DEV + within).reshape(-1).astype(jnp.int32)


def touch_ends(drawn, stream_key, low, largest):
    longest = drawn.shape.index(max(drawn.shape))
    spots = []
    for shift in (0, 1):
        where = [jax.random.randint(jax.random.fold_in(stream_key, axis), (), 0, length) for axis, length in enumerate(drawn.shape)]
        where[longest] = (where[longest] + shift) % drawn.shape[longest]
        spots.append(tuple(where))
    return drawn.at[spots[0]].set(low).at[spots[1]].set(largest)


def level_of(rng, dims, pieces, least, largest):
    factor_of = 1.0
    for position, parts in pieces:
        draws = jax.random.uniform(jax.random.fold_in(jax.random.fold_in(rng, 6), position), (parts,), jnp.float32, least / len(pieces), largest / len(pieces))
        factor_of = factor_of * jnp.repeat(jnp.exp(draws), dims[position] // parts).reshape((-1,) + (1,) * (len(dims) - 1 - position))
    return factor_of


def noise(rng, dims, width, reach, cuts=(), held_as=jnp.bfloat16):
    array = width * jax.random.normal(rng, dims, jnp.float32)
    if cuts:
        array = array * level_of(rng, dims, cuts, -0.22, 0.18)
    return jnp.clip(array, -reach, reach).astype(held_as)


def setup_inputs(seed: int = 0) -> dict:
    splits = jax.random.split(jax.random.key(seed), 7)
    return {
        "occupied": noise(splits[0], (NTAU, NOCC, TILE, TILE), 1.0, 6.0, ((0, 8), (1, 16))),
        "virtual": noise(splits[1], (NTAU, NOCC, TILE, TILE), (TILE * TERMS) ** -0.5, 0.125, ((0, 8), (1, 16))),
        "cos_weights": jnp.clip(jax.random.uniform(splits[2], (NFREQ, NTAU), jnp.float32, -1.0, 1.0), -1.0, 1.0),
        "pair_occ": touch_ends(jax.random.randint(splits[3], (NPART, TERMS), 0, SLOT_DEV), jax.random.fold_in(splits[3], 1), 0, SLOT_DEV - 1).astype(jnp.int32),
        "pair_virt": touch_ends(jax.random.randint(splits[4], (NPART, TERMS), 0, SLOT_DEV), jax.random.fold_in(splits[4], 1), 0, SLOT_DEV - 1).astype(jnp.int32),
        "partial_target_tile": draw_partial_target_tile(jax.random.fold_in(splits[6], 71), 0),
    }


def reference(occupied, virtual, cos_weights, pair_occ, pair_virt, partial_target_tile):
    owner_base = (jnp.arange(NPART, dtype=jnp.int32) // PART_DEV) * SLOT_DEV
    occ_global = (pair_occ + owner_base[:, None]).astype(jnp.int32)
    virt_global = (pair_virt + owner_base[:, None]).astype(jnp.int32)
    group = math.gcd(NPART, 16)
    count = NPART // group
    occ_blocks = occ_global.reshape(count, group, TERMS)
    virt_blocks = virt_global.reshape(count, group, TERMS)
    dest_blocks = partial_target_tile.astype(jnp.int32).reshape(count, group)

    def time_step(spectrum, step_index):
        occ_now = lax.dynamic_index_in_dim(occupied, step_index, 0, keepdims=False)
        virt_now = lax.dynamic_index_in_dim(virtual, step_index, 0, keepdims=False)

        def add_block(chi_time, items):
            left = jnp.take(occ_now, items[0], axis=0).astype(jnp.float32)
            right = jnp.take(virt_now, items[1], axis=0).astype(jnp.float32)
            product = jnp.einsum("bjrk,bjkc->brc", left, right, precision=lax.Precision.HIGHEST)
            return chi_time.at[items[2]].add(product), None

        chi_time, _ = lax.scan(add_block, jnp.zeros((NCHI, TILE, TILE), jnp.float32),
                               (occ_blocks, virt_blocks, dest_blocks))
        weights = lax.dynamic_index_in_dim(cos_weights, step_index, 1, keepdims=False)
        return spectrum + weights[:, None, None, None] * chi_time[None], None

    spectrum, _ = lax.scan(time_step, jnp.zeros((NFREQ, NCHI, TILE, TILE), jnp.float32),
                           jnp.arange(NTAU, dtype=jnp.int32))
    return spectrum
```

```python
import jax
import jax.numpy as jnp
from jax import lax
from jax.experimental import pallas as pl
from jax.experimental.pallas import tpu as pltpu
from jax.sharding import PartitionSpec as P

TILE = 128
SUB = 8
CHI_DEV = 32


def product_kernel(occ_index, virt_index, occupied, virtual, out, *, terms):
    first = pl.program_id(0) * SUB
    flat = out.reshape(TILE * SUB, TILE)
    for q in range(SUB):
        base = (first + q) * terms
        left = jnp.concatenate([occupied[occ_index[base + j]] for j in range(terms)], axis=1)
        right = jnp.concatenate([virtual[virt_index[base + j]] for j in range(terms)], axis=0)
        product = jnp.dot(left, right, preferred_element_type=jnp.float32)
        for i in range(TILE // SUB):
            flat[pl.ds(i * SUB * SUB + q, SUB, stride=SUB), :] = product[i * SUB : (i + 1) * SUB]


def products(occ_index, virt_index, occupied, virtual):
    part, terms = occ_index.shape
    whole = pl.BlockSpec(occupied.shape, lambda g, *_: (0, 0, 0))

    def kernel(*refs):
        product_kernel(*refs, terms=terms)

    return pl.pallas_call(
        kernel,
        out_shape=jax.ShapeDtypeStruct((TILE, part, TILE), jnp.float32),
        grid_spec=pltpu.PrefetchScalarGridSpec(
            num_scalar_prefetch=2,
            grid=(part // SUB,),
            in_specs=[whole, whole],
            out_specs=pl.BlockSpec((TILE, SUB, TILE), lambda g, *_: (0, g, 0)),
        ),
        compiler_params=pltpu.CompilerParams(vmem_limit_bytes=48 * 2**20),
        name="products",
    )(occ_index.reshape(-1), virt_index.reshape(-1), occupied, virtual)


def response_kernel(target, weights, rows, out, even, odd, *, part, chi, nfreq, ntau):
    block = pl.program_id(0)

    @pl.when(block == 0)
    def _():
        even[...] = jnp.zeros_like(even)
        odd[...] = jnp.zeros_like(odd)

    def add(g, carry):
        at = pl.multiple_of(g * SUB, SUB)
        piece = jnp.swapaxes(rows[:, pl.ds(at, SUB), :], 0, 1)
        for q in range(SUB):
            acc = odd if q % 2 else even
            tile = target[block * part + at + q]
            acc[tile] += piece[q]
        return carry

    lax.fori_loop(0, part // SUB, add, 0)

    @pl.when(block == pl.num_programs(0) - 1)
    def _():
        def transform(g, carry):
            at = pl.multiple_of(g * SUB, SUB)
            total = even[pl.ds(at, SUB)] + odd[pl.ds(at, SUB)]
            times = jnp.swapaxes(total, 0, 1)
            owner = g // (CHI_DEV // SUB)
            place = pl.multiple_of((g % (CHI_DEV // SUB)) * SUB, SUB)
            for k in range(nfreq):
                value = weights[k * ntau] * times[0]
                for t in range(1, ntau):
                    value = value + weights[k * ntau + t] * times[t]
                out[owner, k, pl.ds(place, SUB), :] = value
            return carry

        lax.fori_loop(0, chi // SUB, transform, 0)


def responses(target, weights, rows):
    ntau, blocks, part, width = rows.shape
    nfreq = weights.shape[0]
    chi = blocks * CHI_DEV

    def kernel(*refs):
        response_kernel(*refs, part=part, chi=chi, nfreq=nfreq, ntau=ntau)

    return pl.pallas_call(
        kernel,
        out_shape=jax.ShapeDtypeStruct((blocks, nfreq, CHI_DEV, width), jnp.float32),
        grid_spec=pltpu.PrefetchScalarGridSpec(
            num_scalar_prefetch=2,
            grid=(blocks,),
            in_specs=[pl.BlockSpec((ntau, None, part, width), lambda b, *_: (0, b, 0, 0))],
            out_specs=pl.BlockSpec((blocks, nfreq, CHI_DEV, width), lambda b, *_: (0, 0, 0, 0)),
            scratch_shapes=[pltpu.VMEM((chi, ntau, width), jnp.float32)] * 2,
        ),
        compiler_params=pltpu.CompilerParams(vmem_limit_bytes=48 * 2**20),
        name="responses",
    )(target, weights.reshape(-1), rows)


def body(occupied, virtual, cos_weights, pair_occ, pair_virt, partial_target_tile):
    ntau = lax.axis_size("tau")
    blocks = lax.axis_size("tile")
    target = lax.all_gather(partial_target_tile, "tile", tiled=True)
    value = products(pair_occ, pair_virt, occupied[0], virtual[0])
    rows = lax.all_to_all(value, ("tau", "tile"), 0, 0, tiled=True)
    rows = rows.reshape(ntau, blocks, *rows.shape[1:])
    spectrum = responses(target, cos_weights, rows)
    owned = lax.all_to_all(spectrum, "tile", 0, 0, tiled=True)
    return jnp.transpose(owned, (1, 2, 0, 3))


def solution(mesh):
    in_specs = (
        P("tau", "tile", None, None),
        P("tau", "tile", None, None),
        P(),
        P("tile", None),
        P("tile", None),
        P("tile"),
    )
    out_specs = P(None, "tile", "tau", None)
    return jax.shard_map(body, mesh=mesh, in_specs=in_specs, out_specs=out_specs, check_vma=False)
```

```python
import jax
import jax.numpy as jnp
from jax import lax
from jax.experimental import pallas as pl
from jax.experimental.pallas import tpu as pltpu
from jax.sharding import PartitionSpec as P

TILE = 128
SUB = 8
CHI_DEV = 32


def product_kernel(occ_index, virt_index, occupied, virtual, out, *, terms, start):
    first = start + pl.program_id(0) * SUB
    flat = out.reshape(TILE * SUB, TILE)
    for q in range(SUB):
        base = (first + q) * terms
        left = jnp.concatenate([occupied[occ_index[base + j]] for j in range(terms)], axis=1)
        right = jnp.concatenate([virtual[virt_index[base + j]] for j in range(terms)], axis=0)
        product = jnp.dot(left, right, preferred_element_type=jnp.float32)
        for i in range(TILE // SUB):
            flat[pl.ds(i * SUB * SUB + q, SUB, stride=SUB), :] = product[i * SUB : (i + 1) * SUB]


def products(occ_index, virt_index, occupied, virtual, start, part, terms):
    whole = pl.BlockSpec(occupied.shape, lambda g, *_: (0, 0, 0))

    def kernel(*refs):
        product_kernel(*refs, terms=terms, start=start)

    return pl.pallas_call(
        kernel,
        out_shape=jax.ShapeDtypeStruct((TILE, part, TILE), jnp.float32),
        grid_spec=pltpu.PrefetchScalarGridSpec(
            num_scalar_prefetch=2,
            grid=(part // SUB,),
            in_specs=[whole, whole],
            out_specs=pl.BlockSpec((TILE, SUB, TILE), lambda g, *_: (0, g, 0)),
        ),
        compiler_params=pltpu.CompilerParams(vmem_limit_bytes=48 * 2**20),
        name="products",
    )(occ_index, virt_index, occupied, virtual)


def add_kernel(target, rows, *refs, first, part, stride):
    *given, out, even, odd = refs
    block = pl.program_id(0)

    @pl.when(block == 0)
    def _():
        even[...] = given[0][...] if given else jnp.zeros_like(even)
        odd[...] = jnp.zeros_like(odd)

    def add(g, carry):
        at = pl.multiple_of(g * SUB, SUB)
        piece = jnp.swapaxes(rows[:, pl.ds(at, SUB), :], 0, 1)
        for q in range(SUB):
            acc = odd if q % 2 else even
            tile = target[block * stride + first + at + q]
            acc[tile] += piece[q]
        return carry

    lax.fori_loop(0, part // SUB, add, 0)

    @pl.when(block == pl.num_programs(0) - 1)
    def _():
        out[...] = even[...] + odd[...]


def add_rows(target, rows, given, first, stride):
    ntau, blocks, part, width = rows.shape
    chi = (blocks * CHI_DEV, ntau, width)
    whole = pl.BlockSpec(chi, lambda b, *_: (0, 0, 0))

    def kernel(*refs):
        add_kernel(*refs, first=first, part=part, stride=stride)

    return pl.pallas_call(
        kernel,
        out_shape=jax.ShapeDtypeStruct(chi, jnp.float32),
        grid_spec=pltpu.PrefetchScalarGridSpec(
            num_scalar_prefetch=1,
            grid=(blocks,),
            in_specs=[pl.BlockSpec((ntau, None, part, width), lambda b, *_: (0, b, 0, 0))] + [whole] * len(given),
            out_specs=whole,
            scratch_shapes=[pltpu.VMEM(chi, jnp.float32)] * 2,
        ),
        compiler_params=pltpu.CompilerParams(vmem_limit_bytes=48 * 2**20),
        name="add_rows",
    )(target, rows, *given)


def transform_kernel(weights, chi, out, *, nfreq, ntau):
    def step(g, carry):
        at = pl.multiple_of(g * SUB, SUB)
        times = jnp.swapaxes(chi[pl.ds(at, SUB)], 0, 1)
        owner = g // (CHI_DEV // SUB)
        place = pl.multiple_of((g % (CHI_DEV // SUB)) * SUB, SUB)
        for k in range(nfreq):
            value = weights[k * ntau] * times[0]
            for t in range(1, ntau):
                value = value + weights[k * ntau + t] * times[t]
            out[owner, k, pl.ds(place, SUB), :] = value
        return carry

    lax.fori_loop(0, chi.shape[0] // SUB, step, 0)


def transform(weights, chi):
    tiles, ntau, width = chi.shape
    nfreq = weights.shape[0]
    shape = (tiles // CHI_DEV, nfreq, CHI_DEV, width)

    def kernel(*refs):
        transform_kernel(*refs, nfreq=nfreq, ntau=ntau)

    return pl.pallas_call(
        kernel,
        out_shape=jax.ShapeDtypeStruct(shape, jnp.float32),
        grid_spec=pltpu.PrefetchScalarGridSpec(
            num_scalar_prefetch=1,
            grid=(1,),
            in_specs=[pl.BlockSpec(chi.shape, lambda b, *_: (0, 0, 0))],
            out_specs=pl.BlockSpec(shape, lambda b, *_: (0, 0, 0, 0)),
        ),
        compiler_params=pltpu.CompilerParams(vmem_limit_bytes=48 * 2**20),
        name="transform",
    )(weights.reshape(-1), chi)


CHUNKS = (48, 96, 48)


def body(occupied, virtual, cos_weights, pair_occ, pair_virt, partial_target_tile):
    ntau = lax.axis_size("tau")
    blocks = lax.axis_size("tile")
    part, terms = pair_occ.shape
    copies = jnp.broadcast_to(partial_target_tile, (blocks, part))
    target = lax.all_to_all(copies, "tile", 0, 0, tiled=True).reshape(-1)
    target, occ_index, virt_index = lax.optimization_barrier((target, pair_occ.reshape(-1), pair_virt.reshape(-1)))
    first = 0
    arrived = []
    for count in CHUNKS:
        value = products(occ_index, virt_index, occupied[0], virtual[0], first, count, terms)
        rows = lax.all_to_all(value, ("tau", "tile"), 0, 0, tiled=True)
        arrived.append((first, rows.reshape(ntau, blocks, *rows.shape[1:])))
        first += count
    chi = ()
    for first, rows in arrived:
        chi = (add_rows(target, rows, chi, first, part),)
    spectrum = transform(cos_weights, chi[0])
    owned = lax.all_to_all(spectrum, "tile", 0, 0, tiled=True)
    return jnp.transpose(owned, (1, 2, 0, 3))


def solution(mesh):
    in_specs = (
        P("tau", "tile", None, None),
        P("tau", "tile", None, None),
        P(),
        P("tile", None),
        P("tile", None),
        P("tile"),
    )
    out_specs = P(None, "tile", "tau", None)
    return jax.shard_map(body, mesh=mesh, in_specs=in_specs, out_specs=out_specs, check_vma=False)
```

```python
import jax
import jax.numpy as jnp
from jax import lax
from jax.experimental import pallas as pl
from jax.experimental.pallas import tpu as pltpu
from jax.sharding import PartitionSpec as P

TILE = 128
SUB = 8
CHI_DEV = 32
STRIP = 16
TILE_FIRST = 104
GROUP = 7


def shifts(ntau):
    return [(s, h) for s in range(ntau // 2) for h in range(2)]


def partner(me, shift, ntau, back=False):
    s, h = shift
    chips = ntau // 2
    chip = (me // 2 + (chips - s if back else s)) % chips
    core = (me % 2 + h) % 2
    return 2 * chip + core


def product_of(occ_index, virt_index, occupied, virtual, p, terms):
    base = p * terms
    left = jnp.concatenate([occupied[occ_index[base + j]] for j in range(terms)], axis=1)
    right = jnp.concatenate([virtual[virt_index[base + j]] for j in range(terms)], axis=0)
    return jnp.dot(left, right, preferred_element_type=jnp.float32)


def tile_first_kernel(occ_index, virt_index, occupied, virtual, target, out, *, terms, group, strips):
    step = pl.program_id(0)
    flat = out.reshape(strips * group * SUB, TILE)

    def one(q):
        product = product_of(occ_index, virt_index, occupied, virtual, step * group + q, terms)
        for v in range(TILE // SUB):
            r, h = divmod(v, 2)
            flat[pl.ds((h * SUB * group + q) * SUB + r, SUB, stride=group * SUB), :] = product[v * SUB : (v + 1) * SUB]

    for q in range(group - 1):
        one(q)

    @pl.when(step < pl.num_programs(0) - 1)
    def _():
        one(group - 1)

    @pl.when(step == pl.num_programs(0) - 1)
    def _():
        for b in range(strips):
            out[b, group - 1] = target[...]


def tile_first_products(occ_index, virt_index, occupied, virtual, target, count, terms, strips):
    whole = pl.BlockSpec(occupied.shape, lambda g, *_: (0, 0, 0))

    def kernel(*refs):
        tile_first_kernel(*refs, terms=terms, group=GROUP, strips=strips)

    return pl.pallas_call(
        kernel,
        out_shape=jax.ShapeDtypeStruct((strips, count + 1, SUB, TILE), jnp.float32),
        grid_spec=pltpu.PrefetchScalarGridSpec(
            num_scalar_prefetch=2,
            grid=((count + 1) // GROUP,),
            in_specs=[whole, whole, pl.BlockSpec((SUB, TILE), lambda g, *_: (0, 0))],
            out_specs=pl.BlockSpec((strips, GROUP, SUB, TILE), lambda g, *_: (0, g, 0, 0)),
        ),
        compiler_params=pltpu.CompilerParams(vmem_limit_bytes=48 * 2**20),
        name="tile_first_products",
    )(occ_index, virt_index, occupied, virtual, target)


def tau_first_kernel(occ_index, virt_index, occupied, virtual, *refs, terms, start, ntau):
    *outs, whole = refs
    me = lax.axis_index("tau")
    first = start + pl.program_id(0) * SUB
    for q in range(SUB):
        whole[q] = product_of(occ_index, virt_index, occupied, virtual, first + q, terms)
        for out, shift in zip(outs, shifts(ntau)):
            flat = out.reshape(STRIP * SUB, TILE)
            at = pl.multiple_of(partner(me, shift, ntau) * STRIP, STRIP)
            for h in range(STRIP // SUB):
                flat[pl.ds(h * SUB * SUB + q, SUB, stride=SUB), :] = whole[q, pl.ds(at + h * SUB, SUB), :]


def tau_first_products(occ_index, virt_index, occupied, virtual, start, count, terms, ntau):
    whole = pl.BlockSpec(occupied.shape, lambda g, *_: (0, 0, 0))

    def kernel(*refs):
        tau_first_kernel(*refs, terms=terms, start=start, ntau=ntau)

    return pl.pallas_call(
        kernel,
        out_shape=[jax.ShapeDtypeStruct((STRIP, count, TILE), jnp.float32)] * ntau,
        grid_spec=pltpu.PrefetchScalarGridSpec(
            num_scalar_prefetch=2,
            grid=(count // SUB,),
            in_specs=[whole, whole],
            out_specs=[pl.BlockSpec((STRIP, SUB, TILE), lambda g, *_: (0, g, 0))] * ntau,
            scratch_shapes=[pltpu.VMEM((SUB, TILE, TILE), jnp.float32)],
        ),
        compiler_params=pltpu.CompilerParams(vmem_limit_bytes=48 * 2**20),
        name="tau_first_products",
    )(occ_index, virt_index, occupied, virtual)


def weigh_kernel(weights, *refs, ntau, nfreq):
    *strips, out = refs
    me = lax.axis_index("tau")
    times = [partner(me, shift, ntau, back=True) for shift in shifts(ntau)]
    scale = [[weights[k * ntau + t] for t in times] for k in range(nfreq)]
    groups = out.shape[2] // SUB

    def step(i, carry):
        row = i // groups
        at = pl.multiple_of((i % groups) * SUB, SUB)
        values = [strip[row, pl.ds(at, SUB), :] for strip in strips]
        for k in range(nfreq):
            total = scale[k][0] * values[0]
            for t in range(1, ntau):
                total = total + scale[k][t] * values[t]
            out[row, k, pl.ds(at, SUB), :] = total
        return carry

    lax.fori_loop(0, out.shape[0] * groups, step, 0)


def weigh(weights, strips, nfreq):
    ntau = len(strips)
    rows, count, width = strips[0].shape
    per = 4

    def kernel(*refs):
        weigh_kernel(*refs, ntau=ntau, nfreq=nfreq)

    return pl.pallas_call(
        kernel,
        out_shape=jax.ShapeDtypeStruct((rows, nfreq, count, width), jnp.float32),
        grid_spec=pltpu.PrefetchScalarGridSpec(
            num_scalar_prefetch=1,
            grid=(rows // per,),
            in_specs=[pl.BlockSpec((per, count, width), lambda g, *_: (g, 0, 0))] * ntau,
            out_specs=pl.BlockSpec((per, nfreq, count, width), lambda g, *_: (g, 0, 0, 0)),
        ),
        compiler_params=pltpu.CompilerParams(vmem_limit_bytes=48 * 2**20),
        name="weigh",
    )(weights, *strips)


def add_tile_first_kernel(target, rows, out, even, odd, *, count, stride):
    block = pl.program_id(0)

    @pl.when(block == 0)
    def _():
        even[...] = jnp.zeros_like(even)
        odd[...] = jnp.zeros_like(odd)

    def add(g, carry):
        for q in range(SUB):
            acc = odd if q % 2 else even
            p = g * SUB + q
            acc[target[block * stride + p]] += rows[p]
        return carry

    lax.fori_loop(0, count // SUB, add, 0)

    @pl.when(block == pl.num_programs(0) - 1)
    def _():
        def turn(g, carry):
            at = pl.multiple_of(g * SUB, SUB)
            out[:, pl.ds(at, SUB), :] = jnp.swapaxes(even[pl.ds(at, SUB)] + odd[pl.ds(at, SUB)], 0, 1)
            return carry

        lax.fori_loop(0, even.shape[0] // SUB, turn, 0)


def add_tile_first(target, rows, count, stride):
    blocks, slots, ntau, width = rows.shape
    chi = (blocks * CHI_DEV, ntau, width)
    shape = (ntau, blocks * CHI_DEV, width)

    def kernel(*refs):
        add_tile_first_kernel(*refs, count=count, stride=stride)

    return pl.pallas_call(
        kernel,
        out_shape=jax.ShapeDtypeStruct(shape, jnp.float32),
        grid_spec=pltpu.PrefetchScalarGridSpec(
            num_scalar_prefetch=1,
            grid=(blocks,),
            in_specs=[pl.BlockSpec((None, slots, ntau, width), lambda b, *_: (b, 0, 0, 0))],
            out_specs=pl.BlockSpec(shape, lambda b, *_: (0, 0, 0)),
            scratch_shapes=[pltpu.VMEM(chi, jnp.float32)] * 2,
        ),
        compiler_params=pltpu.CompilerParams(vmem_limit_bytes=48 * 2**20),
        name="add_tile_first",
    )(target, rows)


def finish_kernel(target, weights, *refs, starts, stride, ntau, nfreq):
    n = len(starts)
    pieces, (times, out, even, odd) = refs[:n], refs[n:]
    pair = pl.program_id(0)
    lower = lax.broadcasted_iota(jnp.int32, (SUB, TILE), 0) < nfreq

    @pl.when(pair == 0)
    def _():
        even[...] = jnp.zeros_like(even)
        odd[...] = jnp.zeros_like(odd)

    for start, piece in zip(starts, pieces):

        def add(g, carry, start=start, piece=piece):
            at = pl.multiple_of(g * SUB, SUB)
            both = jnp.concatenate([piece[0, :, pl.ds(at, SUB), :], piece[1, :, pl.ds(at, SUB), :]], axis=0)
            both = jnp.swapaxes(both, 0, 1)
            base = 2 * pair * stride + start + at
            for q in range(SUB):
                even[target[base + q]] += jnp.where(lower, both[q], 0.0)
                odd[target[base + stride + q]] += jnp.where(lower, 0.0, both[q])
            return carry

        lax.fori_loop(0, piece.shape[2] // SUB, add, 0)

    @pl.when(pair == pl.num_programs(0) - 1)
    def _():
        def step(g, carry):
            at = pl.multiple_of(g * SUB, SUB)
            total = jnp.swapaxes(even[pl.ds(at, SUB)] + odd[pl.ds(at, SUB)], 0, 1)
            values = [times[t, pl.ds(at, SUB), :] for t in range(ntau)]
            owner = g // (CHI_DEV // SUB)
            place = pl.multiple_of((g % (CHI_DEV // SUB)) * SUB, SUB)
            for k in range(nfreq):
                value = total[k] + total[k + nfreq]
                for t in range(ntau):
                    value = value + weights[k * ntau + t] * values[t]
                out[owner, k, pl.ds(place, SUB), :] = value
            return carry

        lax.fori_loop(0, even.shape[0] // SUB, step, 0)


def finish(target, weights, pieces, starts, times, stride, nfreq):
    ntau, tiles, width = times.shape
    blocks = tiles // CHI_DEV
    shape = (blocks, nfreq, CHI_DEV, width)

    def kernel(*refs):
        finish_kernel(*refs, starts=starts, stride=stride, ntau=ntau, nfreq=nfreq)

    return pl.pallas_call(
        kernel,
        out_shape=jax.ShapeDtypeStruct(shape, jnp.float32),
        grid_spec=pltpu.PrefetchScalarGridSpec(
            num_scalar_prefetch=2,
            grid=(blocks // 2,),
            in_specs=[pl.BlockSpec((2, nfreq, p.shape[2], width), lambda b, *_: (b, 0, 0, 0)) for p in pieces]
            + [pl.BlockSpec(times.shape, lambda b, *_: (0, 0, 0))],
            out_specs=pl.BlockSpec(shape, lambda b, *_: (0, 0, 0, 0)),
            scratch_shapes=[pltpu.VMEM((tiles, SUB, width), jnp.float32)] * 2,
        ),
        compiler_params=pltpu.CompilerParams(vmem_limit_bytes=48 * 2**20),
        name="finish",
    )(target, weights, *pieces, times)


TAU_FIRST = (88,)


def body(occupied, virtual, cos_weights, pair_occ, pair_virt, partial_target_tile):
    ntau = lax.axis_size("tau")
    blocks = lax.axis_size("tile")
    part, terms = pair_occ.shape
    nfreq = cos_weights.shape[0]
    weights = cos_weights.reshape(-1)
    occ_index = pair_occ.reshape(-1)
    virt_index = pair_virt.reshape(-1)
    slot = jnp.pad(partial_target_tile.astype(jnp.float32), (0, SUB * TILE - part)).reshape(SUB, TILE)
    value = tile_first_products(occ_index, virt_index, occupied[0], virtual[0], slot, TILE_FIRST, terms, blocks)
    rows = lax.all_to_all(value, "tile", 0, 0, tiled=True)

    weighted, starts, start = [], [], TILE_FIRST
    for count in TAU_FIRST:
        strips = tau_first_products(occ_index, virt_index, occupied[0], virtual[0], start, count, terms, ntau)
        moved = [strips[0]] + [
            lax.ppermute(strip, "tau", [(i, partner(i, shift, ntau)) for i in range(ntau)])
            for strip, shift in zip(strips[1:], shifts(ntau)[1:])
        ]
        weighted.append(weigh(weights, moved, nfreq))
        starts.append(start)
        start += count

    lines = -(-part // TILE)
    target = rows[:, TILE_FIRST, :lines, :].astype(jnp.int32).reshape(-1)
    stride = lines * TILE
    chi = add_tile_first(target, rows, TILE_FIRST, stride)
    pieces = [lax.all_to_all(w, "tile", 0, 0, tiled=True) for w in weighted]
    times = lax.all_to_all(chi, "tau", 0, 0, tiled=True)
    spectrum = finish(target, weights, pieces, starts, times, stride, nfreq)
    owned = lax.all_to_all(spectrum, "tile", 0, 0, tiled=True)
    return jnp.transpose(owned, (1, 2, 0, 3))


def solution(mesh):
    in_specs = (
        P("tau", "tile", None, None),
        P("tau", "tile", None, None),
        P(),
        P("tile", None),
        P("tile", None),
        P("tile"),
    )
    out_specs = P(None, "tile", "tau", None)
    return jax.shard_map(body, mesh=mesh, in_specs=in_specs, out_specs=out_specs, check_vma=False)
```

```python
import jax
import jax.numpy as jnp
from jax import lax
from jax.experimental import pallas as pl
from jax.experimental.pallas import tpu as pltpu
from jax.sharding import PartitionSpec as P


TILE = 128
SUB = 8
CHI_DEV = 32
STRIP = 16
TILE_FIRST = (48, 56)
TAU_FIRST = 88
GROUP = 7


def shifts(ntau):
    return [(s, h) for s in range(ntau // 2) for h in range(2)]


def partner(me, shift, ntau, back=False):
    s, h = shift
    chips = ntau // 2
    chip = (me // 2 + (chips - s if back else s)) % chips
    core = (me % 2 + h) % 2
    return 2 * chip + core


def product_of(occ_index, virt_index, occupied, virtual, p, terms, offsets):
    base = p * terms
    slots = [occ_index[base + j] for j in range(terms)]
    strips = [jnp.concatenate([occupied[i, pl.ds(at, STRIP), :] for i in slots], axis=1) for at in offsets]
    left = jnp.concatenate(strips, axis=0)
    right = jnp.concatenate([virtual[virt_index[base + j]] for j in range(terms)], axis=0)
    return jnp.dot(left, right, preferred_element_type=jnp.float32)


def load(pairs, arrived):
    copies = [pltpu.make_async_copy(a, b, arrived.at[i]) for i, (a, b) in enumerate(pairs)]
    for copy in copies:
        copy.start()
    for copy in copies:
        copy.wait()


def strip_offsets(ntau):
    me = lax.axis_index("tau")
    return [pl.multiple_of(partner(me, shift, ntau) * STRIP, STRIP) for shift in shifts(ntau)]


def tile_first_kernel(
    occ_index, virt_index, occ_far, virt_far, *refs, terms, group, start, count, strips, ntau
):
    *given, out, occupied, virtual, arrived = refs
    load([(occ_far, occupied), (virt_far, virtual)], arrived)
    slots = out.shape[1]
    flat = out.reshape(strips * slots * SUB, TILE)
    offsets = strip_offsets(ntau)

    def step(g, carry):
        for q in range(group):
            p = jnp.minimum(g * group + q, count - 1)
            product = product_of(occ_index, virt_index, occupied, virtual, start + p, terms, offsets)
            for v in range(TILE // SUB):
                i, h = divmod(v, 2)
                at = (h * SUB * slots + g * group + q) * SUB + i
                flat[pl.ds(at, SUB, stride=slots * SUB), :] = product[v * SUB : (v + 1) * SUB]
        return carry

    lax.fori_loop(0, slots // group, step, 0)
    for target in given:
        for b in range(strips):
            out[b, slots - 1] = target[...]


def tile_first_products(occ_index, virt_index, occupied, virtual, targets, start, count, terms, strips, ntau):
    far = pl.BlockSpec(memory_space=pltpu.HBM)
    store = pltpu.VMEM(occupied.shape, occupied.dtype)
    slots = count + len(targets)

    def kernel(*refs):
        tile_first_kernel(*refs, terms=terms, group=GROUP, start=start, count=count, strips=strips, ntau=ntau)

    return pl.pallas_call(
        kernel,
        out_shape=jax.ShapeDtypeStruct((strips, slots, SUB, TILE), jnp.float32),
        grid_spec=pltpu.PrefetchScalarGridSpec(
            num_scalar_prefetch=2,
            grid=(1,),
            in_specs=[far, far] + [pl.BlockSpec((SUB, TILE), lambda g, *_: (0, 0))] * len(targets),
            out_specs=pl.BlockSpec((strips, slots, SUB, TILE), lambda g, *_: (0, 0, 0, 0)),
            scratch_shapes=[store, store, pltpu.SemaphoreType.DMA((2,))],
        ),
        compiler_params=pltpu.CompilerParams(vmem_limit_bytes=60 * 2**20),
        name="tile_first_products",
    )(occ_index, virt_index, occupied, virtual, *targets)


def tau_first_kernel(occ_index, virt_index, occ_far, virt_far, *refs, terms, start, ntau):
    *outs, occupied, virtual, arrived = refs
    load([(occ_far, occupied), (virt_far, virtual)], arrived)
    offsets = strip_offsets(ntau)
    count = outs[0].shape[1]
    flats = [out.reshape(STRIP * count, TILE) for out in outs]

    def step(g, carry):
        for q in range(SUB):
            p = g * SUB + q
            product = product_of(occ_index, virt_index, occupied, virtual, start + p, terms, offsets)
            for v in range(TILE // SUB):
                i, h = divmod(v, 2)
                flats[i][pl.ds(h * SUB * count + p, SUB, stride=count), :] = product[v * SUB : (v + 1) * SUB]
        return carry

    lax.fori_loop(0, count // SUB, step, 0)


def tau_first_products(occ_index, virt_index, occupied, virtual, start, count, terms, ntau):
    far = pl.BlockSpec(memory_space=pltpu.HBM)
    store = pltpu.VMEM(occupied.shape, occupied.dtype)

    def kernel(*refs):
        tau_first_kernel(*refs, terms=terms, start=start, ntau=ntau)

    return pl.pallas_call(
        kernel,
        out_shape=[jax.ShapeDtypeStruct((STRIP, count, TILE), jnp.float32)] * ntau,
        grid_spec=pltpu.PrefetchScalarGridSpec(
            num_scalar_prefetch=2,
            grid=(1,),
            in_specs=[far, far],
            out_specs=[pl.BlockSpec((STRIP, count, TILE), lambda g, *_: (0, 0, 0))] * ntau,
            scratch_shapes=[store, store, pltpu.SemaphoreType.DMA((2,))],
        ),
        compiler_params=pltpu.CompilerParams(vmem_limit_bytes=60 * 2**20),
        name="tau_first_products",
    )(occ_index, virt_index, occupied, virtual)


def weigh_kernel(weights, *refs, ntau, nfreq):
    *strips, out = refs
    me = lax.axis_index("tau")
    times = [partner(me, shift, ntau, back=True) for shift in shifts(ntau)]
    scale = [[weights[k * ntau + t] for t in times] for k in range(nfreq)]

    def step(row, carry):
        for at in range(0, out.shape[2], SUB):
            values = [strip[row, at : at + SUB, :] for strip in strips]
            for k in range(nfreq):
                total = scale[k][0] * values[0]
                for t in range(1, ntau):
                    total = total + scale[k][t] * values[t]
                out[row, k, at : at + SUB, :] = total
        return carry

    lax.fori_loop(0, out.shape[0], step, 0)


def weigh(weights, strips, nfreq):
    ntau = len(strips)
    rows, count, width = strips[0].shape
    per = 4

    def kernel(*refs):
        weigh_kernel(*refs, ntau=ntau, nfreq=nfreq)

    return pl.pallas_call(
        kernel,
        out_shape=jax.ShapeDtypeStruct((rows, nfreq, count, width), jnp.float32),
        grid_spec=pltpu.PrefetchScalarGridSpec(
            num_scalar_prefetch=1,
            grid=(rows // per,),
            in_specs=[pl.BlockSpec((per, count, width), lambda g, *_: (g, 0, 0))] * ntau,
            out_specs=pl.BlockSpec((per, nfreq, count, width), lambda g, *_: (g, 0, 0, 0)),
        ),
        compiler_params=pltpu.CompilerParams(vmem_limit_bytes=60 * 2**20),
        name="weigh",
    )(weights, *strips)


BLOCKS = 4


def add_tile_first_kernel(target, *refs, spans, stride):
    n = len(spans)
    pieces, outs, sums = refs[:n], refs[n:-BLOCKS], refs[-BLOCKS:]
    step = pl.program_id(0)

    @pl.when(step == 0)
    def _():
        for acc in sums:
            acc[...] = jnp.zeros_like(acc)

    for (start, count), rows in zip(spans, pieces):

        def add(g, carry, start=start, rows=rows):
            for q in range(SUB):
                p = g * SUB + q
                for block, acc in enumerate(sums):
                    acc[target[(step * BLOCKS + block) * stride + start + p]] += rows[block, p]
            return carry

        lax.fori_loop(0, count // SUB, add, 0)

    @pl.when(step == pl.num_programs(0) - 1)
    def _():
        def turn(g, carry):
            at = pl.multiple_of(g * SUB, SUB)
            total = sum([acc[pl.ds(at, SUB)] for acc in sums[1:]], sums[0][pl.ds(at, SUB)])
            total = jnp.swapaxes(total, 0, 1)
            for i, out in enumerate(outs):
                out[pl.ds(at, SUB), :] = total[i]
            return carry

        lax.fori_loop(0, sums[0].shape[0] // SUB, turn, 0)


def add_tile_first(target, pieces, spans, stride):
    blocks, _, ntau, width = pieces[0].shape
    tiles = blocks * CHI_DEV

    def kernel(*refs):
        add_tile_first_kernel(*refs, spans=spans, stride=stride)

    return pl.pallas_call(
        kernel,
        out_shape=[jax.ShapeDtypeStruct((tiles, width), jnp.float32)] * ntau,
        grid_spec=pltpu.PrefetchScalarGridSpec(
            num_scalar_prefetch=1,
            grid=(blocks // BLOCKS,),
            in_specs=[pl.BlockSpec((BLOCKS, *p.shape[1:]), lambda b, *_: (b, 0, 0, 0)) for p in pieces],
            out_specs=[pl.BlockSpec((tiles, width), lambda b, *_: (0, 0))] * ntau,
            scratch_shapes=[pltpu.VMEM((tiles, ntau, width), jnp.float32)] * BLOCKS,
        ),
        compiler_params=pltpu.CompilerParams(vmem_limit_bytes=60 * 2**20),
        name="add_tile_first",
    )(target, *pieces)


def finish_kernel(target, weights, *refs, starts, stride, ntau, nfreq):
    n = len(starts)
    pieces, times, (out, even, odd) = refs[:n], refs[n : n + ntau], refs[n + ntau :]
    pair = pl.program_id(0)
    me = lax.axis_index("tau")
    origins = [partner(me, shift, ntau, back=True) for shift in shifts(ntau)]
    lower = lax.broadcasted_iota(jnp.int32, (SUB, TILE), 0) < nfreq

    @pl.when(pair == 0)
    def _():
        even[...] = jnp.zeros_like(even)
        odd[...] = jnp.zeros_like(odd)

    for start, piece in zip(starts, pieces):

        def add(g, carry, start=start, piece=piece):
            at = pl.multiple_of(g * SUB, SUB)
            both = jnp.concatenate([piece[0, :, pl.ds(at, SUB), :], piece[1, :, pl.ds(at, SUB), :]], axis=0)
            both = jnp.swapaxes(both, 0, 1)
            base = 2 * pair * stride + start + at
            for q in range(SUB):
                even[target[base + q]] += jnp.where(lower, both[q], 0.0)
                odd[target[base + stride + q]] += jnp.where(lower, 0.0, both[q])
            return carry

        lax.fori_loop(0, piece.shape[2] // SUB, add, 0)

    @pl.when(pair == pl.num_programs(0) - 1)
    def _():
        def step(g, carry):
            at = pl.multiple_of(g * SUB, SUB)
            total = jnp.swapaxes(even[pl.ds(at, SUB)] + odd[pl.ds(at, SUB)], 0, 1)
            values = [part[pl.ds(at, SUB), :] for part in times]
            owner = g // (CHI_DEV // SUB)
            place = pl.multiple_of((g % (CHI_DEV // SUB)) * SUB, SUB)
            for k in range(nfreq):
                value = total[k] + total[k + nfreq]
                for t, part in zip(origins, values):
                    value = value + weights[k * ntau + t] * part
                out[owner, k, pl.ds(place, SUB), :] = value
            return carry

        lax.fori_loop(0, even.shape[0] // SUB, step, 0)


def finish(target, weights, pieces, starts, times, stride, nfreq):
    ntau = len(times)
    tiles, width = times[0].shape
    blocks = tiles // CHI_DEV
    shape = (blocks, nfreq, CHI_DEV, width)

    def kernel(*refs):
        finish_kernel(*refs, starts=starts, stride=stride, ntau=ntau, nfreq=nfreq)

    return pl.pallas_call(
        kernel,
        out_shape=jax.ShapeDtypeStruct(shape, jnp.float32),
        grid_spec=pltpu.PrefetchScalarGridSpec(
            num_scalar_prefetch=2,
            grid=(blocks // 2,),
            in_specs=[pl.BlockSpec((2, nfreq, p.shape[2], width), lambda b, *_: (b, 0, 0, 0)) for p in pieces]
            + [pl.BlockSpec((tiles, width), lambda b, *_: (0, 0))] * ntau,
            out_specs=pl.BlockSpec(shape, lambda b, *_: (0, 0, 0, 0)),
            scratch_shapes=[pltpu.VMEM((tiles, SUB, width), jnp.float32)] * 2,
        ),
        compiler_params=pltpu.CompilerParams(vmem_limit_bytes=50 * 2**20),
        name="finish",
    )(target, weights, *pieces, *times)


def over_tau(strips):
    ntau = len(strips)
    return [strips[0]] + [
        lax.ppermute(strip, "tau", [(i, partner(i, shift, ntau)) for i in range(ntau)])
        for strip, shift in zip(strips[1:], shifts(ntau)[1:])
    ]


def body(occupied, virtual, cos_weights, pair_occ, pair_virt, partial_target_tile):
    ntau = lax.axis_size("tau")
    blocks = lax.axis_size("tile")
    part, terms = pair_occ.shape
    nfreq = cos_weights.shape[0]
    weights = cos_weights.reshape(-1)
    occ_index = pair_occ.reshape(-1)
    virt_index = pair_virt.reshape(-1)
    slot = jnp.pad(partial_target_tile.astype(jnp.float32), (0, SUB * TILE - part)).reshape(SUB, TILE)
    stores = occupied[0], virtual[0]
    first, second = TILE_FIRST
    spans = [(0, first), (first + TAU_FIRST, second)]

    value = tile_first_products(occ_index, virt_index, *stores, [slot], *spans[0], terms, blocks, ntau)
    occ_index, value = lax.optimization_barrier((occ_index, value))
    rows = lax.all_to_all(value, "tile", 0, 0, tiled=True)
    strips = list(tau_first_products(occ_index, virt_index, *stores, first, TAU_FIRST, terms, ntau))
    occ_index, strips[0] = lax.optimization_barrier((occ_index, strips[0]))
    strips = over_tau(strips)
    value = tile_first_products(occ_index, virt_index, *stores, [], *spans[1], terms, blocks, ntau)
    value, rows, weights = lax.optimization_barrier((value, rows, weights))
    more = lax.all_to_all(value, "tile", 0, 0, tiled=True)
    weighted = weigh(weights, strips, nfreq)
    weighted, more = lax.optimization_barrier((weighted, more))
    piece = lax.all_to_all(weighted, "tile", 0, 0, tiled=True)

    lines = -(-part // TILE)
    target = rows[:, first, :lines, :].astype(jnp.int32).reshape(-1)
    stride = lines * TILE
    times = over_tau(add_tile_first(target, [rows, more], spans, stride))
    spectrum = finish(target, weights, [piece], [first], times, stride, nfreq)
    owned = lax.all_to_all(spectrum, "tile", 0, 0, tiled=True)
    return jnp.transpose(owned, (1, 2, 0, 3))


def solution(mesh):
    in_specs = (
        P("tau", "tile", None, None),
        P("tau", "tile", None, None),
        P(),
        P("tile", None),
        P("tile", None),
        P("tile"),
    )
    out_specs = P(None, "tile", "tau", None)

    return jax.shard_map(body, mesh=mesh, in_specs=in_specs, out_specs=out_specs, check_vma=False)
```

```python
import jax
import jax.numpy as jnp
from jax import lax
from jax.experimental import pallas as pl
from jax.experimental.pallas import tpu as pltpu
from jax.sharding import PartitionSpec as P


TILE = 128
SUB = 8
CHI_DEV = 32
STRIP = 16
TILE_FIRST = (56, 56)
TAU_FIRST = 80
SIDE = 4


def shifts(ntau):
    return [(s, h) for s in range(ntau // 2) for h in range(2)]


def partner(me, shift, ntau, back=False):
    s, h = shift
    chips = ntau // 2
    chip = (me // 2 + (chips - s if back else s)) % chips
    core = (me % 2 + h) % 2
    return 2 * chip + core


def product_of(occ_index, virt_index, occupied, virtual, p, terms, offsets):
    slots = [occ_index[j, p] for j in range(terms)]
    strips = [jnp.concatenate([occupied[i, pl.ds(at, STRIP), :] for i in slots], axis=1) for at in offsets]
    left = jnp.concatenate(strips, axis=0)
    right = jnp.concatenate([virtual[virt_index[j, p]] for j in range(terms)], axis=0)
    return jnp.dot(left, right, preferred_element_type=jnp.float32)


def load(pairs, arrived):
    copies = [pltpu.make_async_copy(a, b, arrived.at[i]) for i, (a, b) in enumerate(pairs)]
    for copy in copies:
        copy.start()
    for copy in copies:
        copy.wait()


def strip_offsets(ntau):
    me = lax.axis_index("tau")
    return [pl.multiple_of(partner(me, shift, ntau) * STRIP, STRIP) for shift in shifts(ntau)]


def around(me, s, u, z_first, back=False):
    dz, dy = (s, u) if z_first else (u, s)
    z, y = me // SIDE, me % SIDE
    if back:
        return (z + SIDE - dz) % SIDE * SIDE + (y + SIDE - dy) % SIDE
    return (z + dz) % SIDE * SIDE + (y + dy) % SIDE


def tile_first_kernel(occ_index, virt_index, occ_far, virt_far, *refs, terms, start, count, ntau, z_first, given):
    target, outs, (rows, occupied, virtual, arrived, left) = refs[:given], refs[given : given + SIDE], refs[given + SIDE :]
    load([(occ_far, occupied), (virt_far, virtual)], arrived)
    strips, slots = rows.shape[:2]
    flat = rows.reshape(strips * slots * SUB, TILE)
    offsets = strip_offsets(ntau)

    def step(g, carry):
        for q in range(SUB):
            p = g * SUB + q
            product = product_of(occ_index, virt_index, occupied, virtual, start + p, terms, offsets)
            for v in range(TILE // SUB):
                i, h = divmod(v, 2)
                at = (h * SUB * slots + p) * SUB + i
                flat[pl.ds(at, SUB, stride=slots * SUB), :] = product[v * SUB : (v + 1) * SUB]
        return carry

    lax.fori_loop(0, count // SUB, step, 0)
    for ref in target:
        for b in range(strips):
            rows[b, count] = ref[...]
    me = lax.axis_index("tile")
    copies = []
    for s in range(SIDE):
        for u in range(SIDE):
            source = rows.at[around(me, s, u, z_first), pl.ds(0, count + given)]
            copies.append(pltpu.make_async_copy(source, outs[s].at[u], left.at[s * SIDE + u]))
    for copy in copies:
        copy.start()
    for copy in copies:
        copy.wait()


def tile_first_products(occ_index, virt_index, occupied, virtual, targets, start, count, terms, strips, ntau, z_first):
    far = pl.BlockSpec(memory_space=pltpu.HBM)
    store = pltpu.VMEM(occupied.shape, occupied.dtype)
    given = len(targets)

    def kernel(*refs):
        tile_first_kernel(*refs, terms=terms, start=start, count=count, ntau=ntau, z_first=z_first, given=given)

    return pl.pallas_call(
        kernel,
        out_shape=[jax.ShapeDtypeStruct((SIDE, count + given, SUB, TILE), jnp.float32)] * SIDE,
        grid_spec=pltpu.PrefetchScalarGridSpec(
            num_scalar_prefetch=2,
            grid=(1,),
            in_specs=[far, far] + [pl.BlockSpec((SUB, TILE), lambda g, *_: (0, 0))] * given,
            out_specs=[far] * SIDE,
            scratch_shapes=[
                pltpu.VMEM((strips, count + 1, SUB, TILE), jnp.float32),
                store,
                store,
                pltpu.SemaphoreType.DMA((2,)),
                pltpu.SemaphoreType.DMA((strips,)),
            ],
        ),
        compiler_params=pltpu.CompilerParams(vmem_limit_bytes=60 * 2**20),
        name="tile_first_products",
    )(occ_index, virt_index, occupied, virtual, *targets)


def tau_first_kernel(occ_index, virt_index, occ_far, virt_far, *refs, terms, start, ntau):
    *outs, occupied, virtual, arrived = refs
    load([(occ_far, occupied), (virt_far, virtual)], arrived)
    offsets = strip_offsets(ntau)
    count = outs[0].shape[1]
    flats = [out.reshape(STRIP * count, TILE) for out in outs]

    def step(g, carry):
        for q in range(SUB):
            p = g * SUB + q
            product = product_of(occ_index, virt_index, occupied, virtual, start + p, terms, offsets)
            for v in range(TILE // SUB):
                i, h = divmod(v, 2)
                flats[i][pl.ds(h * SUB * count + p, SUB, stride=count), :] = product[v * SUB : (v + 1) * SUB]
        return carry

    lax.fori_loop(0, count // SUB, step, 0)


def tau_first_products(occ_index, virt_index, occupied, virtual, start, count, terms, ntau):
    far = pl.BlockSpec(memory_space=pltpu.HBM)
    store = pltpu.VMEM(occupied.shape, occupied.dtype)

    def kernel(*refs):
        tau_first_kernel(*refs, terms=terms, start=start, ntau=ntau)

    return pl.pallas_call(
        kernel,
        out_shape=[jax.ShapeDtypeStruct((STRIP, count, TILE), jnp.float32)] * ntau,
        grid_spec=pltpu.PrefetchScalarGridSpec(
            num_scalar_prefetch=2,
            grid=(1,),
            in_specs=[far, far],
            out_specs=[pl.BlockSpec((STRIP, count, TILE), lambda g, *_: (0, 0, 0))] * ntau,
            scratch_shapes=[store, store, pltpu.SemaphoreType.DMA((2,))],
        ),
        compiler_params=pltpu.CompilerParams(vmem_limit_bytes=60 * 2**20),
        name="tau_first_products",
    )(occ_index, virt_index, occupied, virtual)


def weigh_kernel(weights, *refs, ntau, nfreq):
    *strips, out = refs
    me = lax.axis_index("tau")
    times = [partner(me, shift, ntau, back=True) for shift in shifts(ntau)]
    scale = [[weights[k * ntau + t] for t in times] for k in range(nfreq)]

    def step(row, carry):
        for at in range(0, out.shape[2], SUB):
            values = [strip[row, at : at + SUB, :] for strip in strips]
            for k in range(nfreq):
                total = scale[k][0] * values[0]
                for t in range(1, ntau):
                    total = total + scale[k][t] * values[t]
                out[row, k, at : at + SUB, :] = total
        return carry

    lax.fori_loop(0, out.shape[0], step, 0)


def weigh(weights, strips, nfreq):
    ntau = len(strips)
    rows, count, width = strips[0].shape
    per = 4

    def kernel(*refs):
        weigh_kernel(*refs, ntau=ntau, nfreq=nfreq)

    return pl.pallas_call(
        kernel,
        out_shape=jax.ShapeDtypeStruct((rows, nfreq, count, width), jnp.float32),
        grid_spec=pltpu.PrefetchScalarGridSpec(
            num_scalar_prefetch=1,
            grid=(rows // per,),
            in_specs=[pl.BlockSpec((per, count, width), lambda g, *_: (g, 0, 0))] * ntau,
            out_specs=pl.BlockSpec((per, nfreq, count, width), lambda g, *_: (g, 0, 0, 0)),
        ),
        compiler_params=pltpu.CompilerParams(vmem_limit_bytes=60 * 2**20),
        name="weigh",
    )(weights, *strips)


def add_tile_first_kernel(target, *refs, spans, stride, ntau):
    sums, outs = refs[-SIDE:], refs[-SIDE - ntau : -SIDE]
    for acc in sums:
        acc[...] = jnp.zeros_like(acc)
    for half, (start, count) in enumerate(spans):
        near, far = refs[half * (2 * SIDE - 1) :][:SIDE], refs[half * (2 * SIDE - 1) + SIDE :][: SIDE - 1]
        for u in range(SIDE):
            rows = [far[u - 1].at[s] if u else near[s].at[0] for s in range(SIDE)]
            places = [(s, u) if half == 0 else (u, s) for s in range(SIDE)]
            bases = [(dz * SIDE + dy) * stride + start for dz, dy in places]

            def add(g, carry, rows=rows, bases=bases):
                for q in range(SUB):
                    p = g * SUB + q
                    for ref, base, acc in zip(rows, bases, sums):
                        acc[target[base + p]] += ref[p]
                return carry

            lax.fori_loop(0, count // SUB, add, 0)

    def turn(g, carry):
        at = pl.multiple_of(g * SUB, SUB)
        total = sum([acc[pl.ds(at, SUB)] for acc in sums[1:]], sums[0][pl.ds(at, SUB)])
        total = jnp.swapaxes(total, 0, 1)
        for i, out in enumerate(outs):
            out[pl.ds(at, SUB), :] = total[i]
        return carry

    lax.fori_loop(0, sums[0].shape[0] // SUB, turn, 0)


def add_tile_first(target, halves, spans, stride, ntau):
    tiles = SIDE * SIDE * CHI_DEV
    operands, specs = [], []
    for near, far in halves:
        operands += [*near, *far]
        specs += [pl.BlockSpec((1, *p.shape[1:]), lambda b, *_: (0, 0, 0, 0)) for p in near]
        specs += [pl.BlockSpec(p.shape, lambda b, *_: (0, 0, 0, 0)) for p in far]

    def kernel(*refs):
        add_tile_first_kernel(*refs, spans=spans, stride=stride, ntau=ntau)

    return pl.pallas_call(
        kernel,
        out_shape=[jax.ShapeDtypeStruct((tiles, TILE), jnp.float32)] * ntau,
        grid_spec=pltpu.PrefetchScalarGridSpec(
            num_scalar_prefetch=1,
            grid=(1,),
            in_specs=specs,
            out_specs=[pl.BlockSpec((tiles, TILE), lambda b, *_: (0, 0))] * ntau,
            scratch_shapes=[pltpu.VMEM((tiles, ntau, TILE), jnp.float32)] * SIDE,
        ),
        compiler_params=pltpu.CompilerParams(vmem_limit_bytes=60 * 2**20),
        name="add_tile_first",
    )(target, *operands)


def finish_kernel(target, weights, piece, *refs, start, stride, ntau, nfreq):
    times, out, sums = refs[:ntau], refs[ntau], refs[ntau + 1 :]
    step = pl.program_id(0)
    here = lax.axis_index("tau")
    origins = [partner(here, shift, ntau, back=True) for shift in shifts(ntau)]
    lower = lax.broadcasted_iota(jnp.int32, (SUB, TILE), 0) < nfreq
    me = lax.axis_index("tile")
    dz = (me // SIDE + SIDE - step) % SIDE
    bases = [(dz * SIDE + (me % SIDE + SIDE - y) % SIDE) * stride + start for y in range(SIDE)]

    @pl.when(step == 0)
    def _():
        for acc in sums:
            acc[...] = jnp.zeros_like(acc)

    def add(g, carry):
        at = pl.multiple_of(g * SUB, SUB)
        blocks = [piece[i, :, pl.ds(at, SUB), :] for i in range(SIDE)]
        pairs = [jnp.swapaxes(jnp.concatenate(blocks[i : i + 2], axis=0), 0, 1) for i in (0, 2)]
        for q in range(SUB):
            for i in range(SIDE):
                both = pairs[i // 2][q]
                mine = jnp.where(lower, 0.0, both) if i % 2 else jnp.where(lower, both, 0.0)
                sums[i][target[bases[i] + at + q]] += mine
        return carry

    lax.fori_loop(0, piece.shape[2] // SUB, add, 0)

    @pl.when(step == pl.num_programs(0) - 1)
    def _():
        def last(g, carry):
            at = pl.multiple_of(g * SUB, SUB)
            total = sum([acc[pl.ds(at, SUB)] for acc in sums[1:]], sums[0][pl.ds(at, SUB)])
            total = jnp.swapaxes(total, 0, 1)
            values = [part[pl.ds(at, SUB), :] for part in times]
            owner = g // (CHI_DEV // SUB)
            place = pl.multiple_of((g % (CHI_DEV // SUB)) * SUB, SUB)
            for k in range(nfreq):
                value = total[k] + total[k + nfreq]
                for t, part in zip(origins, values):
                    value = value + weights[k * ntau + t] * part
                out[owner, k, pl.ds(place, SUB), :] = value
            return carry

        lax.fori_loop(0, sums[0].shape[0] // SUB, last, 0)


def finish(target, weights, piece, start, times, stride, nfreq):
    ntau = len(times)
    tiles, width = times[0].shape
    blocks = tiles // CHI_DEV
    shape = (blocks, nfreq, CHI_DEV, width)

    def kernel(*refs):
        finish_kernel(*refs, start=start, stride=stride, ntau=ntau, nfreq=nfreq)

    return pl.pallas_call(
        kernel,
        out_shape=jax.ShapeDtypeStruct(shape, jnp.float32),
        grid_spec=pltpu.PrefetchScalarGridSpec(
            num_scalar_prefetch=2,
            grid=(blocks // SIDE,),
            in_specs=[pl.BlockSpec((SIDE, nfreq, piece.shape[2], width), lambda b, *_: (b, 0, 0, 0))]
            + [pl.BlockSpec((tiles, width), lambda b, *_: (0, 0))] * ntau,
            out_specs=pl.BlockSpec(shape, lambda b, *_: (0, 0, 0, 0)),
            scratch_shapes=[pltpu.VMEM((tiles, SUB, width), jnp.float32)] * SIDE,
        ),
        compiler_params=pltpu.CompilerParams(vmem_limit_bytes=50 * 2**20),
        name="finish",
    )(target, weights, piece, *times)


def turn_kernel(*refs):
    near, outs, arrived = refs[:SIDE], refs[SIDE:-1], refs[-1]
    copies = []
    for u in range(1, SIDE):
        for s in range(SIDE):
            copies.append(pltpu.make_async_copy(near[s].at[u], outs[u - 1].at[s], arrived.at[(u - 1) * SIDE + s]))
    for copy in copies:
        copy.start()
    for copy in copies:
        copy.wait()


def turn(near):
    anywhere = pl.BlockSpec(memory_space=pltpu.HBM)
    return pl.pallas_call(
        turn_kernel,
        out_shape=[jax.ShapeDtypeStruct(near[0].shape, jnp.float32)] * (SIDE - 1),
        in_specs=[anywhere] * SIDE,
        out_specs=[anywhere] * (SIDE - 1),
        scratch_shapes=[pltpu.SemaphoreType.DMA((SIDE * (SIDE - 1),))],
        compiler_params=pltpu.CompilerParams(vmem_limit_bytes=60 * 2**20),
        name="turn",
    )(*near)


def over_tau(strips):
    ntau = len(strips)
    return [strips[0]] + [
        lax.ppermute(strip, "tau", [(i, partner(i, shift, ntau)) for i in range(ntau)])
        for strip, shift in zip(strips[1:], shifts(ntau)[1:])
    ]


def over_tile(rows, s, u, z_first):
    n = SIDE * SIDE
    return lax.ppermute(rows, "tile", [(i, around(i, s, u, z_first)) for i in range(n)])


def body(occupied, virtual, cos_weights, pair_occ, pair_virt, partial_target_tile):
    ntau = lax.axis_size("tau")
    blocks = lax.axis_size("tile")
    part, terms = pair_occ.shape
    nfreq = cos_weights.shape[0]
    weights = cos_weights.reshape(-1)
    occ_index = pair_occ.T
    virt_index = pair_virt.T
    slot = jnp.pad(partial_target_tile.astype(jnp.float32), (0, SUB * TILE - part)).reshape(SUB, TILE)
    stores = occupied[0], virtual[0]
    first, second = TILE_FIRST
    spans = [(0, first), (first, second)]

    near, far = [], []
    for half, (start, count) in enumerate(spans):
        outs = list(
            tile_first_products(
                occ_index, virt_index, *stores, [] if half else [slot], start, count, terms, blocks, ntau, half == 0
            )
        )
        occ_index, outs[0] = lax.optimization_barrier((occ_index, outs[0]))
        near.append([outs[0]] + [over_tile(outs[s], s, 0, half == 0) for s in range(1, SIDE)])
    strips = list(tau_first_products(occ_index, virt_index, *stores, first + second, TAU_FIRST, terms, ntau))
    strips = over_tau(strips)
    for half in range(2):
        far.append([over_tile(rows, 0, u + 1, half == 0) for u, rows in enumerate(turn(near[half]))])
    weighted = weigh(weights, strips, nfreq)
    piece = lax.all_to_all(weighted, "tile", 0, 0, tiled=True)

    lines = -(-part // TILE)
    stride = lines * TILE
    by_u = [jnp.stack([n[0, first, :lines] for n in near[0]])] + [f[:, first, :lines] for f in far[0]]
    target = jnp.stack(by_u, axis=1).astype(jnp.int32).reshape(-1)
    chi = add_tile_first(target, list(zip(near, far)), spans, stride, ntau)
    times = over_tau(chi)
    spectrum = finish(target, weights, piece, first + second, times, stride, nfreq)
    owned = lax.all_to_all(spectrum, "tile", 0, 0, tiled=True)
    return jnp.transpose(owned, (1, 2, 0, 3))


def solution(mesh):
    in_specs = (
        P("tau", "tile", None, None),
        P("tau", "tile", None, None),
        P(),
        P("tile", None),
        P("tile", None),
        P("tile"),
    )
    out_specs = P(None, "tile", "tau", None)

    return jax.shard_map(body, mesh=mesh, in_specs=in_specs, out_specs=out_specs, check_vma=False)
```

```python
import jax
import jax.numpy as jnp
from jax import lax
from jax.experimental import pallas as pl
from jax.experimental.pallas import tpu as pltpu
from jax.sharding import PartitionSpec as P


TILE = 128
SUB = 8
CHI_DEV = 32
STRIP = 16
TILE_FIRST = (56, 56)
TAU_FIRST = 80
SIDE = 4


def shifts(ntau):
    return [(s, h) for s in range(ntau // 2) for h in range(2)]


def partner(me, shift, ntau, back=False):
    s, h = shift
    chips = ntau // 2
    chip = (me // 2 + (chips - s if back else s)) % chips
    core = (me % 2 + h) % 2
    return 2 * chip + core


def product_of(occ_index, virt_index, occupied, virtual, p, terms, offsets):
    slots = [occ_index[j, p] for j in range(terms)]
    strips = [jnp.concatenate([occupied[i, pl.ds(at, STRIP), :] for i in slots], axis=1) for at in offsets]
    left = jnp.concatenate(strips, axis=0)
    right = jnp.concatenate([virtual[virt_index[j, p]] for j in range(terms)], axis=0)
    return jnp.dot(left, right, preferred_element_type=jnp.float32)


def load(pairs, arrived):
    copies = [pltpu.make_async_copy(a, b, arrived.at[i]) for i, (a, b) in enumerate(pairs)]
    for copy in copies:
        copy.start()
    for copy in copies:
        copy.wait()


def strip_offsets(ntau):
    me = lax.axis_index("tau")
    return [pl.multiple_of(partner(me, shift, ntau) * STRIP, STRIP) for shift in shifts(ntau)]


def around(me, s, u, z_first, back=False):
    dz, dy = (s, u) if z_first else (u, s)
    z, y = me // SIDE, me % SIDE
    if back:
        return (z + SIDE - dz) % SIDE * SIDE + (y + SIDE - dy) % SIDE
    return (z + dz) % SIDE * SIDE + (y + dy) % SIDE


def tile_first_kernel(occ_index, virt_index, occ_far, virt_far, target, *refs, terms, spans, ntau):
    n = len(spans) * SIDE
    outs, halves, (occupied, virtual, arrived, left) = refs[:n], refs[n : n + len(spans)], refs[n + len(spans) :]
    load([(occ_far, occupied), (virt_far, virtual)], arrived)
    offsets = strip_offsets(ntau)
    me = lax.axis_index("tile")
    copies = []
    for half, ((start, count), rows) in enumerate(zip(spans, halves)):
        strips, slots = rows.shape[:2]
        flat = rows.reshape(strips * slots * SUB, TILE)

        def step(g, carry, start=start, slots=slots, flat=flat):
            for q in range(SUB):
                p = g * SUB + q
                product = product_of(occ_index, virt_index, occupied, virtual, start + p, terms, offsets)
                for v in range(TILE // SUB):
                    i, h = divmod(v, 2)
                    at = (h * SUB * slots + p) * SUB + i
                    flat[pl.ds(at, SUB, stride=slots * SUB), :] = product[v * SUB : (v + 1) * SUB]
            return carry

        lax.fori_loop(0, count // SUB, step, 0)
        if half == 0:
            for b in range(strips):
                rows[b, count] = target[...]
        for s in range(SIDE):
            for u in range(SIDE):
                out = outs[half * SIDE + s]
                source = rows.at[around(me, s, u, half == 0), pl.ds(0, out.shape[1])]
                copies.append(pltpu.make_async_copy(source, out.at[u], left.at[len(copies)]))
                copies[-1].start()
    for copy in copies:
        copy.wait()


def tile_first_products(occ_index, virt_index, occupied, virtual, target, spans, terms, strips, ntau):
    far = pl.BlockSpec(memory_space=pltpu.HBM)
    store = pltpu.VMEM(occupied.shape, occupied.dtype)

    def kernel(*refs):
        tile_first_kernel(*refs, terms=terms, spans=spans, ntau=ntau)

    sizes = [count + (half == 0) for half, (_, count) in enumerate(spans)]
    return pl.pallas_call(
        kernel,
        out_shape=[jax.ShapeDtypeStruct((SIDE, n, SUB, TILE), jnp.float32) for n in sizes for _ in range(SIDE)],
        grid_spec=pltpu.PrefetchScalarGridSpec(
            num_scalar_prefetch=2,
            grid=(1,),
            in_specs=[far, far, pl.BlockSpec((SUB, TILE), lambda g, *_: (0, 0))],
            out_specs=[far] * (SIDE * len(spans)),
            scratch_shapes=[pltpu.VMEM((strips, count + 1, SUB, TILE), jnp.float32) for _, count in spans]
            + [store, store, pltpu.SemaphoreType.DMA((2,)), pltpu.SemaphoreType.DMA((strips * len(spans),))],
        ),
        compiler_params=pltpu.CompilerParams(vmem_limit_bytes=60 * 2**20),
        name="tile_first_products",
    )(occ_index, virt_index, occupied, virtual, target)


def tau_first_kernel(occ_index, virt_index, occ_far, virt_far, *refs, terms, start, ntau):
    *outs, occupied, virtual, arrived = refs
    load([(occ_far, occupied), (virt_far, virtual)], arrived)
    offsets = strip_offsets(ntau)
    count = outs[0].shape[1]
    flats = [out.reshape(STRIP * count, TILE) for out in outs]

    def step(g, carry):
        for q in range(SUB):
            p = g * SUB + q
            product = product_of(occ_index, virt_index, occupied, virtual, start + p, terms, offsets)
            for v in range(TILE // SUB):
                i, h = divmod(v, 2)
                flats[i][pl.ds(h * SUB * count + p, SUB, stride=count), :] = product[v * SUB : (v + 1) * SUB]
        return carry

    lax.fori_loop(0, count // SUB, step, 0)


def tau_first_products(occ_index, virt_index, occupied, virtual, start, count, terms, ntau):
    far = pl.BlockSpec(memory_space=pltpu.HBM)
    store = pltpu.VMEM(occupied.shape, occupied.dtype)

    def kernel(*refs):
        tau_first_kernel(*refs, terms=terms, start=start, ntau=ntau)

    return pl.pallas_call(
        kernel,
        out_shape=[jax.ShapeDtypeStruct((STRIP, count, TILE), jnp.float32)] * ntau,
        grid_spec=pltpu.PrefetchScalarGridSpec(
            num_scalar_prefetch=2,
            grid=(1,),
            in_specs=[far, far],
            out_specs=[pl.BlockSpec((STRIP, count, TILE), lambda g, *_: (0, 0, 0))] * ntau,
            scratch_shapes=[store, store, pltpu.SemaphoreType.DMA((2,))],
        ),
        compiler_params=pltpu.CompilerParams(vmem_limit_bytes=60 * 2**20),
        name="tau_first_products",
    )(occ_index, virt_index, occupied, virtual)


def weigh_kernel(weights, *refs, ntau, nfreq):
    *strips, out = refs
    me = lax.axis_index("tau")
    times = [partner(me, shift, ntau, back=True) for shift in shifts(ntau)]
    scale = [[weights[k * ntau + t] for t in times] for k in range(nfreq)]

    def step(row, carry):
        for at in range(0, out.shape[2], SUB):
            values = [strip[row, at : at + SUB, :] for strip in strips]
            for k in range(nfreq):
                total = scale[k][0] * values[0]
                for t in range(1, ntau):
                    total = total + scale[k][t] * values[t]
                out[row, k, at : at + SUB, :] = total
        return carry

    lax.fori_loop(0, out.shape[0], step, 0)


def weigh(weights, strips, nfreq):
    ntau = len(strips)
    rows, count, width = strips[0].shape
    per = 4

    def kernel(*refs):
        weigh_kernel(*refs, ntau=ntau, nfreq=nfreq)

    return pl.pallas_call(
        kernel,
        out_shape=jax.ShapeDtypeStruct((rows, nfreq, count, width), jnp.float32),
        grid_spec=pltpu.PrefetchScalarGridSpec(
            num_scalar_prefetch=1,
            grid=(rows // per,),
            in_specs=[pl.BlockSpec((per, count, width), lambda g, *_: (g, 0, 0))] * ntau,
            out_specs=pl.BlockSpec((per, nfreq, count, width), lambda g, *_: (g, 0, 0, 0)),
        ),
        compiler_params=pltpu.CompilerParams(vmem_limit_bytes=60 * 2**20),
        name="weigh",
    )(weights, *strips)


def add_tile_first_kernel(target, *refs, spans, stride, ntau):
    sums, outs = refs[-SIDE:], refs[-SIDE - ntau : -SIDE]
    for acc in sums:
        acc[...] = jnp.zeros_like(acc)
    for half, (start, count) in enumerate(spans):
        near, far = refs[half * (2 * SIDE - 1) :][:SIDE], refs[half * (2 * SIDE - 1) + SIDE :][: SIDE - 1]
        for u in range(SIDE):
            rows = [far[u - 1].at[s] if u else near[s].at[0] for s in range(SIDE)]
            places = [(s, u) if half == 0 else (u, s) for s in range(SIDE)]
            bases = [(dz * SIDE + dy) * stride + start for dz, dy in places]

            def add(g, carry, rows=rows, bases=bases):
                for q in range(SUB):
                    p = g * SUB + q
                    for ref, base, acc in zip(rows, bases, sums):
                        acc[target[base + p]] += ref[p]
                return carry

            lax.fori_loop(0, count // SUB, add, 0)

    def turn(g, carry):
        at = pl.multiple_of(g * SUB, SUB)
        total = sum([acc[pl.ds(at, SUB)] for acc in sums[1:]], sums[0][pl.ds(at, SUB)])
        total = jnp.swapaxes(total, 0, 1)
        for i, out in enumerate(outs):
            out[pl.ds(at, SUB), :] = total[i]
        return carry

    lax.fori_loop(0, sums[0].shape[0] // SUB, turn, 0)


def add_tile_first(target, halves, spans, stride, ntau):
    tiles = SIDE * SIDE * CHI_DEV
    operands, specs = [], []
    for near, far in halves:
        operands += [*near, *far]
        specs += [pl.BlockSpec((1, *p.shape[1:]), lambda b, *_: (0, 0, 0, 0)) for p in near]
        specs += [pl.BlockSpec(p.shape, lambda b, *_: (0, 0, 0, 0)) for p in far]

    def kernel(*refs):
        add_tile_first_kernel(*refs, spans=spans, stride=stride, ntau=ntau)

    return pl.pallas_call(
        kernel,
        out_shape=[jax.ShapeDtypeStruct((tiles, TILE), jnp.float32)] * ntau,
        grid_spec=pltpu.PrefetchScalarGridSpec(
            num_scalar_prefetch=1,
            grid=(1,),
            in_specs=specs,
            out_specs=[pl.BlockSpec((tiles, TILE), lambda b, *_: (0, 0))] * ntau,
            scratch_shapes=[pltpu.VMEM((tiles, ntau, TILE), jnp.float32)] * SIDE,
        ),
        compiler_params=pltpu.CompilerParams(vmem_limit_bytes=60 * 2**20),
        name="add_tile_first",
    )(target, *operands)


def finish_kernel(target, weights, piece, *refs, start, stride, ntau, nfreq):
    times, out, sums = refs[:ntau], refs[ntau], refs[ntau + 1 :]
    step = pl.program_id(0)
    here = lax.axis_index("tau")
    origins = [partner(here, shift, ntau, back=True) for shift in shifts(ntau)]
    lower = lax.broadcasted_iota(jnp.int32, (SUB, TILE), 0) < nfreq
    me = lax.axis_index("tile")
    dz = (me // SIDE + SIDE - step) % SIDE
    bases = [(dz * SIDE + (me % SIDE + SIDE - y) % SIDE) * stride + start for y in range(SIDE)]

    @pl.when(step == 0)
    def _():
        for acc in sums:
            acc[...] = jnp.zeros_like(acc)

    def add(g, carry):
        at = pl.multiple_of(g * SUB, SUB)
        blocks = [piece[i, :, pl.ds(at, SUB), :] for i in range(SIDE)]
        pairs = [jnp.swapaxes(jnp.concatenate(blocks[i : i + 2], axis=0), 0, 1) for i in (0, 2)]
        for q in range(SUB):
            for i in range(SIDE):
                both = pairs[i // 2][q]
                mine = jnp.where(lower, 0.0, both) if i % 2 else jnp.where(lower, both, 0.0)
                sums[i][target[bases[i] + at + q]] += mine
        return carry

    lax.fori_loop(0, piece.shape[2] // SUB, add, 0)

    @pl.when(step == pl.num_programs(0) - 1)
    def _():
        def last(g, carry):
            at = pl.multiple_of(g * SUB, SUB)
            total = sum([acc[pl.ds(at, SUB)] for acc in sums[1:]], sums[0][pl.ds(at, SUB)])
            total = jnp.swapaxes(total, 0, 1)
            values = [part[pl.ds(at, SUB), :] for part in times]
            owner = g // (CHI_DEV // SUB)
            place = pl.multiple_of((g % (CHI_DEV // SUB)) * SUB, SUB)
            for k in range(nfreq):
                value = total[k] + total[k + nfreq]
                for t, part in zip(origins, values):
                    value = value + weights[k * ntau + t] * part
                out[owner, k, pl.ds(place, SUB), :] = value
            return carry

        lax.fori_loop(0, sums[0].shape[0] // SUB, last, 0)


def finish(target, weights, piece, start, times, stride, nfreq):
    ntau = len(times)
    tiles, width = times[0].shape
    blocks = tiles // CHI_DEV
    shape = (blocks, nfreq, CHI_DEV, width)

    def kernel(*refs):
        finish_kernel(*refs, start=start, stride=stride, ntau=ntau, nfreq=nfreq)

    return pl.pallas_call(
        kernel,
        out_shape=jax.ShapeDtypeStruct(shape, jnp.float32),
        grid_spec=pltpu.PrefetchScalarGridSpec(
            num_scalar_prefetch=2,
            grid=(blocks // SIDE,),
            in_specs=[pl.BlockSpec((SIDE, nfreq, piece.shape[2], width), lambda b, *_: (b, 0, 0, 0))]
            + [pl.BlockSpec((tiles, width), lambda b, *_: (0, 0))] * ntau,
            out_specs=pl.BlockSpec(shape, lambda b, *_: (0, 0, 0, 0)),
            scratch_shapes=[pltpu.VMEM((tiles, SUB, width), jnp.float32)] * SIDE,
        ),
        compiler_params=pltpu.CompilerParams(vmem_limit_bytes=50 * 2**20),
        name="finish",
    )(target, weights, piece, *times)


def turn_kernel(*refs):
    near, outs, held, arrived, left = refs[:SIDE], refs[SIDE:-3], *refs[-3:]
    inward = []
    for u in range(1, SIDE):
        for s in range(SIDE):
            at = (u - 1) * SIDE + s
            inward.append(pltpu.make_async_copy(near[s].at[u], held.at[u - 1, s], arrived.at[at]))
    outward = [pltpu.make_async_copy(held.at[u], out, left.at[u]) for u, out in enumerate(outs)]
    for copy in inward:
        copy.start()
    for u, copy in enumerate(outward):
        for s in range(SIDE):
            inward[u * SIDE + s].wait()
        copy.start()
    for copy in outward:
        copy.wait()


def turn(near):
    anywhere = pl.BlockSpec(memory_space=pltpu.HBM)
    return pl.pallas_call(
        turn_kernel,
        out_shape=[jax.ShapeDtypeStruct(near[0].shape, jnp.float32)] * (SIDE - 1),
        in_specs=[anywhere] * SIDE,
        out_specs=[anywhere] * (SIDE - 1),
        scratch_shapes=[
            pltpu.VMEM((SIDE - 1, *near[0].shape), jnp.float32),
            pltpu.SemaphoreType.DMA((SIDE * (SIDE - 1),)),
            pltpu.SemaphoreType.DMA((SIDE - 1,)),
        ],
        compiler_params=pltpu.CompilerParams(vmem_limit_bytes=60 * 2**20),
        name="turn",
    )(*near)


def over_tau(strips):
    ntau = len(strips)
    return [strips[0]] + [
        lax.ppermute(strip, "tau", [(i, partner(i, shift, ntau)) for i in range(ntau)])
        for strip, shift in zip(strips[1:], shifts(ntau)[1:])
    ]


def over_tile(rows, s, u, z_first):
    n = SIDE * SIDE
    return lax.ppermute(rows, "tile", [(i, around(i, s, u, z_first)) for i in range(n)])


def body(occupied, virtual, cos_weights, pair_occ, pair_virt, partial_target_tile):
    ntau = lax.axis_size("tau")
    blocks = lax.axis_size("tile")
    part, terms = pair_occ.shape
    nfreq = cos_weights.shape[0]
    weights = cos_weights.reshape(-1)
    occ_index = pair_occ.T
    virt_index = pair_virt.T
    slot = jnp.pad(partial_target_tile.astype(jnp.float32), (0, SUB * TILE - part)).reshape(SUB, TILE)
    stores = occupied[0], virtual[0]
    first, second = TILE_FIRST
    spans = [(0, first), (first, second)]

    near, far = [], []
    outs = list(tile_first_products(occ_index, virt_index, *stores, slot, spans, terms, blocks, ntau))
    occ_index, outs[0] = lax.optimization_barrier((occ_index, outs[0]))
    for half in range(2):
        mine, *others = outs[half * SIDE : (half + 1) * SIDE]
        near.append([mine] + [over_tile(rows, s + 1, 0, half == 0) for s, rows in enumerate(others)])
    strips = list(tau_first_products(occ_index, virt_index, *stores, first + second, TAU_FIRST, terms, ntau))
    strips = over_tau(strips)
    for half in range(2):
        far.append([over_tile(rows, 0, u + 1, half == 0) for u, rows in enumerate(turn(near[half]))])
    weighted = weigh(weights, strips, nfreq)
    piece = lax.all_to_all(weighted, "tile", 0, 0, tiled=True)

    lines = -(-part // TILE)
    stride = lines * TILE
    by_u = [jnp.stack([n[0, first, :lines] for n in near[0]])] + [f[:, first, :lines] for f in far[0]]
    target = jnp.stack(by_u, axis=1).astype(jnp.int32).reshape(-1)
    chi = add_tile_first(target, list(zip(near, far)), spans, stride, ntau)
    times = over_tau(chi)
    spectrum = finish(target, weights, piece, first + second, times, stride, nfreq)
    owned = lax.all_to_all(spectrum, "tile", 0, 0, tiled=True)
    return jnp.transpose(owned, (1, 2, 0, 3))


def solution(mesh):
    in_specs = (
        P("tau", "tile", None, None),
        P("tau", "tile", None, None),
        P(),
        P("tile", None),
        P("tile", None),
        P("tile"),
    )
    out_specs = P(None, "tile", "tau", None)

    return jax.shard_map(body, mesh=mesh, in_specs=in_specs, out_specs=out_specs, check_vma=False)
```

```python
import jax
import jax.numpy as jnp
from jax import lax
from jax.experimental import pallas as pl
from jax.experimental.pallas import tpu as pltpu
from jax.sharding import PartitionSpec as P


TILE = 128
SUB = 8
CHI_DEV = 32
STRIP = 16
TILE_FIRST = (48, 64)
TAU_FIRST = 80
SIDE = 4


def shifts(ntau):
    return [(s, h) for s in range(ntau // 2) for h in range(2)]


def partner(me, shift, ntau, back=False):
    s, h = shift
    chips = ntau // 2
    chip = (me // 2 + (chips - s if back else s)) % chips
    core = (me % 2 + h) % 2
    return 2 * chip + core


def product_of(occ_index, virt_index, occupied, virtual, p, terms):
    left = jnp.concatenate([occupied[occ_index[j, p]] for j in range(terms)], axis=1)
    right = jnp.concatenate([virtual[virt_index[j, p]] for j in range(terms)], axis=0)
    return jnp.dot(left, right, preferred_element_type=jnp.float32)


def load(pairs, arrived):
    copies = [pltpu.make_async_copy(a, b, arrived.at[i]) for i, (a, b) in enumerate(pairs)]
    for copy in copies:
        copy.start()
    for copy in copies:
        copy.wait()


def around(me, s, u, z_first, back=False):
    dz, dy = (s, u) if z_first else (u, s)
    z, y = me // SIDE, me % SIDE
    if back:
        return (z + SIDE - dz) % SIDE * SIDE + (y + SIDE - dy) % SIDE
    return (z + dz) % SIDE * SIDE + (y + dy) % SIDE


def tile_first_kernel(occ_index, virt_index, occ_far, virt_far, target, *refs, terms, spans):
    n = len(spans) * SIDE
    outs, halves, (occupied, virtual, arrived, left) = refs[:n], refs[n : n + len(spans)], refs[n + len(spans) :]
    load([(occ_far, occupied), (virt_far, virtual)], arrived)
    me = lax.axis_index("tile")
    copies = []
    for half, ((start, count), rows) in enumerate(zip(spans, halves)):
        strips, slots = rows.shape[:2]
        flat = rows.reshape(strips * slots * SUB, TILE)

        def step(g, carry, start=start, slots=slots, flat=flat):
            for q in range(SUB):
                p = g * SUB + q
                product = product_of(occ_index, virt_index, occupied, virtual, start + p, terms)
                for v in range(TILE // SUB):
                    i, h = divmod(v, 2)
                    at = (h * SUB * slots + p) * SUB + i
                    flat[pl.ds(at, SUB, stride=slots * SUB), :] = product[v * SUB : (v + 1) * SUB]
            return carry

        lax.fori_loop(0, count // SUB, step, 0)
        if half == 0:
            for b in range(strips):
                rows[b, count] = target[...]
        for s in range(SIDE):
            for u in range(SIDE):
                out = outs[half * SIDE + s]
                source = rows.at[around(me, s, u, half == 0), pl.ds(0, out.shape[1])]
                copies.append(pltpu.make_async_copy(source, out.at[u], left.at[len(copies)]))
                copies[-1].start()
    for copy in copies:
        copy.wait()


def tile_first_products(occ_index, virt_index, occupied, virtual, target, spans, terms, strips):
    far = pl.BlockSpec(memory_space=pltpu.HBM)
    store = pltpu.VMEM(occupied.shape, occupied.dtype)

    def kernel(*refs):
        tile_first_kernel(*refs, terms=terms, spans=spans)

    sizes = [count + (half == 0) for half, (_, count) in enumerate(spans)]
    return pl.pallas_call(
        kernel,
        out_shape=[jax.ShapeDtypeStruct((SIDE, n, SUB, TILE), jnp.float32) for n in sizes for _ in range(SIDE)],
        grid_spec=pltpu.PrefetchScalarGridSpec(
            num_scalar_prefetch=2,
            grid=(1,),
            in_specs=[far, far, pl.BlockSpec((SUB, TILE), lambda g, *_: (0, 0))],
            out_specs=[far] * (SIDE * len(spans)),
            scratch_shapes=[pltpu.VMEM((strips, count + 1, SUB, TILE), jnp.float32) for _, count in spans]
            + [store, store, pltpu.SemaphoreType.DMA((2,)), pltpu.SemaphoreType.DMA((strips * len(spans),))],
        ),
        compiler_params=pltpu.CompilerParams(vmem_limit_bytes=60 * 2**20),
        name="tile_first_products",
    )(occ_index, virt_index, occupied, virtual, target)


def tau_first_kernel(occ_index, virt_index, occ_far, virt_far, *refs, terms, start, count, ntau):
    outs, (strips, occupied, virtual, arrived, left) = refs[:ntau], refs[ntau:]
    load([(occ_far, occupied), (virt_far, virtual)], arrived)
    slots = strips.shape[2]
    flat = strips.reshape(ntau * STRIP * slots, TILE)

    def step(g, carry):
        for q in range(SUB):
            p = g * SUB + q
            product = product_of(occ_index, virt_index, occupied, virtual, start + p, terms)
            for v in range(TILE // SUB):
                flat[pl.ds(v * SUB * slots + p, SUB, stride=slots), :] = product[v * SUB : (v + 1) * SUB]
        return carry

    lax.fori_loop(0, count // SUB, step, 0)
    me = lax.axis_index("tau")
    copies = []
    for i, shift in enumerate(shifts(ntau)):
        source = strips.at[partner(me, shift, ntau), :, pl.ds(0, count)]
        copies.append(pltpu.make_async_copy(source, outs[i], left.at[i]))
    for copy in copies:
        copy.start()
    for copy in copies:
        copy.wait()


def tau_first_products(occ_index, virt_index, occupied, virtual, start, count, terms, ntau):
    far = pl.BlockSpec(memory_space=pltpu.HBM)
    store = pltpu.VMEM(occupied.shape, occupied.dtype)
    slots = count if count // SUB % 2 else count + SUB

    def kernel(*refs):
        tau_first_kernel(*refs, terms=terms, start=start, count=count, ntau=ntau)

    return pl.pallas_call(
        kernel,
        out_shape=[jax.ShapeDtypeStruct((STRIP, count, TILE), jnp.float32)] * ntau,
        grid_spec=pltpu.PrefetchScalarGridSpec(
            num_scalar_prefetch=2,
            grid=(1,),
            in_specs=[far, far],
            out_specs=[far] * ntau,
            scratch_shapes=[
                pltpu.VMEM((ntau, STRIP, slots, TILE), jnp.float32),
                store,
                store,
                pltpu.SemaphoreType.DMA((2,)),
                pltpu.SemaphoreType.DMA((ntau,)),
            ],
        ),
        compiler_params=pltpu.CompilerParams(vmem_limit_bytes=60 * 2**20),
        name="tau_first_products",
    )(occ_index, virt_index, occupied, virtual)


def weigh_kernel(weights, *refs, ntau, nfreq):
    *strips, out = refs
    me = lax.axis_index("tau")
    times = [partner(me, shift, ntau, back=True) for shift in shifts(ntau)]
    scale = [[jnp.full((SUB, TILE), weights[k * ntau + t], jnp.float32) for t in times] for k in range(nfreq)]

    def step(row, carry):
        for at in range(0, out.shape[2], SUB):
            values = [strip[row, at : at + SUB, :] for strip in strips]
            for k in range(nfreq):
                total = scale[k][0] * values[0]
                for t in range(1, ntau):
                    total = total + scale[k][t] * values[t]
                out[row, k, at : at + SUB, :] = total
        return carry

    lax.fori_loop(0, out.shape[0], step, 0)


def weigh(weights, strips, nfreq):
    ntau = len(strips)
    rows, count, width = strips[0].shape
    per = 4

    def kernel(*refs):
        weigh_kernel(*refs, ntau=ntau, nfreq=nfreq)

    return pl.pallas_call(
        kernel,
        out_shape=jax.ShapeDtypeStruct((rows, nfreq, count, width), jnp.float32),
        grid_spec=pltpu.PrefetchScalarGridSpec(
            num_scalar_prefetch=1,
            grid=(rows // per,),
            in_specs=[pl.BlockSpec((per, count, width), lambda g, *_: (g, 0, 0))] * ntau,
            out_specs=pl.BlockSpec((per, nfreq, count, width), lambda g, *_: (g, 0, 0, 0)),
        ),
        compiler_params=pltpu.CompilerParams(vmem_limit_bytes=60 * 2**20),
        name="weigh",
    )(weights, *strips)


def add_tile_first_kernel(target, *refs, spans, stride, ntau):
    *refs, turned = refs
    n = 2 * SIDE
    sums, outs = refs[-n:], refs[-n - ntau : -n]
    me = lax.axis_index("tau")
    order = [partner(me, shift, ntau) for shift in shifts(ntau)]
    for acc in sums:
        acc[...] = jnp.zeros_like(acc)
    work = []
    for half, (start, count) in enumerate(spans):
        near, far = refs[half * (2 * SIDE - 1) :][:SIDE], refs[half * (2 * SIDE - 1) + SIDE :][: SIDE - 1]
        for u in range(SIDE):
            rows = [far[u - 1].at[s] if u else near[s].at[0] for s in range(SIDE)]
            places = [(s, u) if half == 0 else (u, s) for s in range(SIDE)]
            bases = [(dz * SIDE + dy) * stride + start for dz, dy in places]

            work.append((rows, bases, count))
    for u in range(SIDE):
        first, second = work[u], work[u + SIDE]
        both = (first[0] + second[0], first[1] + second[1])
        middle, end = sorted((first[2] // SUB, second[2] // SUB))
        longer = max(first, second, key=lambda item: item[2])
        for (rows, bases), low, high in ((both, 0, middle), (longer[:2], middle, end)):

            def add(g, carry, rows=rows, bases=bases):
                for q in range(SUB):
                    p = g * SUB + q
                    for ref, base, acc in zip(rows, bases, sums):
                        acc[target[base + p]] += ref[p]
                return carry

            if low < high:
                lax.fori_loop(low, high, add, 0)

    def turn(g, carry):
        at = pl.multiple_of(g * SUB, SUB)
        total = sum([acc[pl.ds(at, SUB)] for acc in sums[1:]], sums[0][pl.ds(at, SUB)])
        turned[:, pl.ds(at, SUB), :] = jnp.swapaxes(total, 0, 1)
        return carry

    lax.fori_loop(0, sums[0].shape[0] // SUB, turn, 0)
    for r, out in zip(order, outs):
        out[...] = turned[r]


def add_tile_first(target, halves, spans, stride, ntau):
    tiles = SIDE * SIDE * CHI_DEV
    operands, specs = [], []
    for near, far in halves:
        operands += [*near, *far]
        specs += [pl.BlockSpec((1, *p.shape[1:]), lambda b, *_: (0, 0, 0, 0)) for p in near]
        specs += [pl.BlockSpec(p.shape, lambda b, *_: (0, 0, 0, 0)) for p in far]

    def kernel(*refs):
        add_tile_first_kernel(*refs, spans=spans, stride=stride, ntau=ntau)

    return pl.pallas_call(
        kernel,
        out_shape=[jax.ShapeDtypeStruct((tiles, TILE), jnp.float32)] * ntau,
        grid_spec=pltpu.PrefetchScalarGridSpec(
            num_scalar_prefetch=1,
            grid=(1,),
            in_specs=specs,
            out_specs=[pl.BlockSpec((tiles, TILE), lambda b, *_: (0, 0))] * ntau,
            scratch_shapes=[pltpu.VMEM((tiles, ntau, TILE), jnp.float32)] * (2 * SIDE)
            + [pltpu.VMEM((ntau, tiles, TILE), jnp.float32)],
        ),
        compiler_params=pltpu.CompilerParams(vmem_limit_bytes=60 * 2**20),
        name="add_tile_first",
    )(target, *operands)


def finish_kernel(target, weights, piece, *refs, start, stride, ntau, nfreq):
    times, out, sums = refs[:ntau], refs[ntau], refs[ntau + 1 :]
    step = pl.program_id(0)
    here = lax.axis_index("tau")
    origins = [partner(here, shift, ntau, back=True) for shift in shifts(ntau)]
    lower = lax.broadcasted_iota(jnp.int32, (SUB, TILE), 0) < nfreq
    me = lax.axis_index("tile")
    dz = (me // SIDE + SIDE - step) % SIDE
    bases = [(dz * SIDE + (me % SIDE + SIDE - y) % SIDE) * stride + start for y in range(SIDE)]

    @pl.when(step == 0)
    def _():
        for acc in sums:
            acc[...] = jnp.zeros_like(acc)

    def add(g, carry):
        at = pl.multiple_of(g * SUB, SUB)
        blocks = [piece[i, :, pl.ds(at, SUB), :] for i in range(SIDE)]
        pairs = [jnp.swapaxes(jnp.concatenate(blocks[i : i + 2], axis=0), 0, 1) for i in (0, 2)]
        for q in range(SUB):
            for i in range(SIDE):
                both = pairs[i // 2][q]
                mine = jnp.where(lower, 0.0, both) if i % 2 else jnp.where(lower, both, 0.0)
                sums[i][target[bases[i] + at + q]] += mine
        return carry

    lax.fori_loop(0, piece.shape[2] // SUB, add, 0)

    @pl.when(step == pl.num_programs(0) - 1)
    def _():
        scale = [[jnp.full((SUB, TILE), weights[k * ntau + t], jnp.float32) for t in origins] for k in range(nfreq)]

        def last(g, carry):
            at = pl.multiple_of(g * SUB, SUB)
            total = sum([acc[pl.ds(at, SUB)] for acc in sums[1:]], sums[0][pl.ds(at, SUB)])
            total = jnp.swapaxes(total, 0, 1)
            values = [part[pl.ds(at, SUB), :] for part in times]
            owner = g // (CHI_DEV // SUB)
            place = pl.multiple_of((g % (CHI_DEV // SUB)) * SUB, SUB)
            for k in range(nfreq):
                value = total[k] + total[k + nfreq]
                for factor, part in zip(scale[k], values):
                    value = value + factor * part
                out[owner, k, pl.ds(place, SUB), :] = value
            return carry

        lax.fori_loop(0, sums[0].shape[0] // SUB, last, 0)


def finish(target, weights, piece, start, times, stride, nfreq):
    ntau = len(times)
    tiles, width = times[0].shape
    blocks = tiles // CHI_DEV
    shape = (blocks, nfreq, CHI_DEV, width)

    def kernel(*refs):
        finish_kernel(*refs, start=start, stride=stride, ntau=ntau, nfreq=nfreq)

    return pl.pallas_call(
        kernel,
        out_shape=jax.ShapeDtypeStruct(shape, jnp.float32),
        grid_spec=pltpu.PrefetchScalarGridSpec(
            num_scalar_prefetch=2,
            grid=(blocks // SIDE,),
            in_specs=[pl.BlockSpec((SIDE, nfreq, piece.shape[2], width), lambda b, *_: (b, 0, 0, 0))]
            + [pl.BlockSpec((tiles, width), lambda b, *_: (0, 0))] * ntau,
            out_specs=pl.BlockSpec(shape, lambda b, *_: (0, 0, 0, 0)),
            scratch_shapes=[pltpu.VMEM((tiles, SUB, width), jnp.float32)] * SIDE,
        ),
        compiler_params=pltpu.CompilerParams(vmem_limit_bytes=50 * 2**20),
        name="finish",
    )(target, weights, piece, *times)


def turn_kernel(*refs):
    near, outs, held, arrived, left = refs[:SIDE], refs[SIDE:-3], *refs[-3:]
    inward = []
    for u in range(1, SIDE):
        for s in range(SIDE):
            at = (u - 1) * SIDE + s
            inward.append(pltpu.make_async_copy(near[s].at[u], held.at[u - 1, s], arrived.at[at]))
    outward = [pltpu.make_async_copy(held.at[u], out, left.at[u]) for u, out in enumerate(outs)]
    for copy in inward:
        copy.start()
    for u, copy in enumerate(outward):
        for s in range(SIDE):
            inward[u * SIDE + s].wait()
        copy.start()
    for copy in outward:
        copy.wait()


def turn(near):
    anywhere = pl.BlockSpec(memory_space=pltpu.HBM)
    return pl.pallas_call(
        turn_kernel,
        out_shape=[jax.ShapeDtypeStruct(near[0].shape, jnp.float32)] * (SIDE - 1),
        in_specs=[pl.BlockSpec(memory_space=pl.ANY)] * SIDE,
        out_specs=[anywhere] * (SIDE - 1),
        scratch_shapes=[
            pltpu.VMEM((SIDE - 1, *near[0].shape), jnp.float32),
            pltpu.SemaphoreType.DMA((SIDE * (SIDE - 1),)),
            pltpu.SemaphoreType.DMA((SIDE - 1,)),
        ],
        compiler_params=pltpu.CompilerParams(vmem_limit_bytes=60 * 2**20),
        name="turn",
    )(*near)


def over_tau(strips):
    ntau = len(strips)
    return [strips[0]] + [
        lax.ppermute(strip, "tau", [(i, partner(i, shift, ntau)) for i in range(ntau)])
        for strip, shift in zip(strips[1:], shifts(ntau)[1:])
    ]


def over_tile(rows, s, u, z_first):
    n = SIDE * SIDE
    return lax.ppermute(rows, "tile", [(i, around(i, s, u, z_first)) for i in range(n)])


def body(occupied, virtual, cos_weights, pair_occ, pair_virt, partial_target_tile):
    ntau = lax.axis_size("tau")
    blocks = lax.axis_size("tile")
    part, terms = pair_occ.shape
    nfreq = cos_weights.shape[0]
    weights = cos_weights.reshape(-1)
    occ_index = pair_occ.T
    virt_index = pair_virt.T
    slot = jnp.pad(partial_target_tile.astype(jnp.float32), (0, SUB * TILE - part)).reshape(SUB, TILE)
    stores = occupied[0], virtual[0]
    first, second = TILE_FIRST
    spans = [(0, first), (first, second)]

    near, far = [], []
    outs = list(tile_first_products(occ_index, virt_index, *stores, slot, spans, terms, blocks))
    occ_index, outs[0] = lax.optimization_barrier((occ_index, outs[0]))
    for half in range(2):
        mine, *others = outs[half * SIDE : (half + 1) * SIDE]
        near.append([mine] + [over_tile(rows, s + 1, 0, half == 0) for s, rows in enumerate(others)])
    strips = list(tau_first_products(occ_index, virt_index, *stores, first + second, TAU_FIRST, terms, ntau))
    strips = over_tau(strips)
    for half in range(2):
        far.append([over_tile(rows, 0, u + 1, half == 0) for u, rows in enumerate(turn(near[half]))])
    weighted = weigh(weights, strips, nfreq)
    piece = lax.all_to_all(weighted, "tile", 0, 0, tiled=True)

    lines = -(-part // TILE)
    stride = lines * TILE
    by_u = [jnp.stack([n[0, first, :lines] for n in near[0]])] + [f[:, first, :lines] for f in far[0]]
    target = jnp.stack(by_u, axis=1).astype(jnp.int32).reshape(-1)
    chi = add_tile_first(target, list(zip(near, far)), spans, stride, ntau)
    times = over_tau(chi)
    spectrum = finish(target, weights, piece, first + second, times, stride, nfreq)
    owned = lax.all_to_all(spectrum, "tile", 0, 0, tiled=True)
    return jnp.transpose(owned, (1, 2, 0, 3))


def solution(mesh):
    in_specs = (
        P("tau", "tile", None, None),
        P("tau", "tile", None, None),
        P(),
        P("tile", None),
        P("tile", None),
        P("tile"),
    )
    out_specs = P(None, "tile", "tau", None)

    return jax.shard_map(body, mesh=mesh, in_specs=in_specs, out_specs=out_specs, check_vma=False)
```

```python
import jax
import jax.numpy as jnp
from jax import lax
from jax.experimental import pallas as pl
from jax.experimental.pallas import tpu as pltpu
from jax.sharding import PartitionSpec as P


TILE = 128
SUB = 8
CHI_DEV = 32
STRIP = 16
TILE_FIRST = (56, 56)
TAU_FIRST = 80
SIDE = 4


def shifts(ntau):
    chips = ntau // 2
    far_first = sorted(range(chips), key=lambda s: (s > 0, -min(s, chips - s)))
    return [(s, h) for s in far_first for h in range(2)]


def partner(me, shift, ntau, back=False):
    s, h = shift
    chips = ntau // 2
    chip = (me // 2 + (chips - s if back else s)) % chips
    core = (me % 2 + h) % 2
    return 2 * chip + core


def product_of(occ_index, virt_index, occupied, virtual, p, terms):
    left = jnp.concatenate([occupied[occ_index[j, p]] for j in range(terms)], axis=1)
    right = jnp.concatenate([virtual[virt_index[j, p]] for j in range(terms)], axis=0)
    return jnp.dot(left, right, preferred_element_type=jnp.float32)


def load(pairs, arrived):
    copies = [pltpu.make_async_copy(a, b, arrived.at[i]) for i, (a, b) in enumerate(pairs)]
    for copy in copies:
        copy.start()
    for copy in copies:
        copy.wait()


def around(me, s, u, z_first, back=False):
    dz, dy = (s, u) if z_first else (u, s)
    z, y = me // SIDE, me % SIDE
    if back:
        return (z + SIDE - dz) % SIDE * SIDE + (y + SIDE - dy) % SIDE
    return (z + dz) % SIDE * SIDE + (y + dy) % SIDE


def tile_first_kernel(occ_index, virt_index, occ_far, virt_far, target, *refs, terms, spans):
    n = len(spans) * SIDE
    outs, halves, (occupied, virtual, arrived, left) = refs[:n], refs[n : n + len(spans)], refs[n + len(spans) :]
    load([(occ_far, occupied), (virt_far, virtual)], arrived)
    me = lax.axis_index("tile")
    copies = []
    for half, ((start, count), rows) in enumerate(zip(spans, halves)):
        strips, slots = rows.shape[:2]
        flat = rows.reshape(strips * slots * SUB, TILE)

        def step(g, carry, start=start, slots=slots, flat=flat):
            for q in range(SUB):
                p = g * SUB + q
                product = product_of(occ_index, virt_index, occupied, virtual, start + p, terms)
                for v in range(TILE // SUB):
                    i, h = divmod(v, 2)
                    at = (h * SUB * slots + p) * SUB + i
                    flat[pl.ds(at, SUB, stride=slots * SUB), :] = product[v * SUB : (v + 1) * SUB]
            return carry

        lax.fori_loop(0, count // SUB, step, 0)
        if half == 0:
            for b in range(strips):
                rows[b, count] = target[...]
        for s in range(SIDE):
            for u in range(SIDE):
                out = outs[half * SIDE + s]
                source = rows.at[around(me, s, u, half == 0), pl.ds(0, out.shape[1])]
                copies.append(pltpu.make_async_copy(source, out.at[u], left.at[len(copies)]))
                copies[-1].start()
    for copy in copies:
        copy.wait()


def tile_first_products(occ_index, virt_index, occupied, virtual, target, spans, terms, strips):
    far = pl.BlockSpec(memory_space=pltpu.HBM)
    store = pltpu.VMEM(occupied.shape, occupied.dtype)

    def kernel(*refs):
        tile_first_kernel(*refs, terms=terms, spans=spans)

    sizes = [count + (half == 0) for half, (_, count) in enumerate(spans)]
    return pl.pallas_call(
        kernel,
        out_shape=[jax.ShapeDtypeStruct((SIDE, n, SUB, TILE), jnp.float32) for n in sizes for _ in range(SIDE)],
        grid_spec=pltpu.PrefetchScalarGridSpec(
            num_scalar_prefetch=2,
            grid=(1,),
            in_specs=[far, far, pl.BlockSpec((SUB, TILE), lambda g, *_: (0, 0))],
            out_specs=[far] * (SIDE * len(spans)),
            scratch_shapes=[pltpu.VMEM((strips, count + 1, SUB, TILE), jnp.float32) for _, count in spans]
            + [store, store, pltpu.SemaphoreType.DMA((2,)), pltpu.SemaphoreType.DMA((strips * len(spans),))],
        ),
        compiler_params=pltpu.CompilerParams(vmem_limit_bytes=60 * 2**20),
        name="tile_first_products",
    )(occ_index, virt_index, occupied, virtual, target)


def tau_first_kernel(occ_index, virt_index, occ_far, virt_far, *refs, terms, start, count, ntau):
    outs, (strips, occupied, virtual, arrived, left) = refs[:ntau], refs[ntau:]
    load([(occ_far, occupied), (virt_far, virtual)], arrived)
    slots = strips.shape[2]
    flat = strips.reshape(ntau * STRIP * slots, TILE)

    def step(g, carry):
        for q in range(SUB):
            p = g * SUB + q
            product = product_of(occ_index, virt_index, occupied, virtual, start + p, terms)
            for v in range(TILE // SUB):
                flat[pl.ds(v * SUB * slots + p, SUB, stride=slots), :] = product[v * SUB : (v + 1) * SUB]
        return carry

    lax.fori_loop(0, count // SUB, step, 0)
    me = lax.axis_index("tau")
    copies = []
    for i, shift in enumerate(shifts(ntau)):
        source = strips.at[partner(me, shift, ntau), :, pl.ds(0, count)]
        copies.append(pltpu.make_async_copy(source, outs[i], left.at[i]))
    for copy in copies:
        copy.start()
    for copy in copies:
        copy.wait()


def tau_first_products(occ_index, virt_index, occupied, virtual, start, count, terms, ntau):
    far = pl.BlockSpec(memory_space=pltpu.HBM)
    store = pltpu.VMEM(occupied.shape, occupied.dtype)
    slots = count if count // SUB % 2 else count + SUB

    def kernel(*refs):
        tau_first_kernel(*refs, terms=terms, start=start, count=count, ntau=ntau)

    return pl.pallas_call(
        kernel,
        out_shape=[jax.ShapeDtypeStruct((STRIP, count, TILE), jnp.float32)] * ntau,
        grid_spec=pltpu.PrefetchScalarGridSpec(
            num_scalar_prefetch=2,
            grid=(1,),
            in_specs=[far, far],
            out_specs=[far] * ntau,
            scratch_shapes=[
                pltpu.VMEM((ntau, STRIP, slots, TILE), jnp.float32),
                store,
                store,
                pltpu.SemaphoreType.DMA((2,)),
                pltpu.SemaphoreType.DMA((ntau,)),
            ],
        ),
        compiler_params=pltpu.CompilerParams(vmem_limit_bytes=60 * 2**20),
        name="tau_first_products",
    )(occ_index, virt_index, occupied, virtual)


def weigh_kernel(weights, *refs, ntau, nfreq):
    *strips, out = refs
    me = lax.axis_index("tau")
    times = [partner(me, shift, ntau, back=True) for shift in shifts(ntau)]
    scale = [[jnp.full((SUB, TILE), weights[k * ntau + t], jnp.float32) for t in times] for k in range(nfreq)]

    def step(row, carry):
        for at in range(0, out.shape[2], SUB):
            values = [strip[row, at : at + SUB, :] for strip in strips]
            for k in range(nfreq):
                total = scale[k][0] * values[0]
                for t in range(1, ntau):
                    total = total + scale[k][t] * values[t]
                out[row, k, at : at + SUB, :] = total
        return carry

    lax.fori_loop(0, out.shape[0], step, 0)


def weigh(weights, strips, nfreq):
    ntau = len(strips)
    rows, count, width = strips[0].shape
    per = 4

    def kernel(*refs):
        weigh_kernel(*refs, ntau=ntau, nfreq=nfreq)

    return pl.pallas_call(
        kernel,
        out_shape=jax.ShapeDtypeStruct((rows, nfreq, count, width), jnp.float32),
        grid_spec=pltpu.PrefetchScalarGridSpec(
            num_scalar_prefetch=1,
            grid=(rows // per,),
            in_specs=[pl.BlockSpec((per, count, width), lambda g, *_: (g, 0, 0))] * ntau,
            out_specs=pl.BlockSpec((per, nfreq, count, width), lambda g, *_: (g, 0, 0, 0)),
        ),
        compiler_params=pltpu.CompilerParams(vmem_limit_bytes=60 * 2**20),
        name="weigh",
    )(weights, *strips)


def add_tile_first_kernel(target, *refs, spans, stride, ntau):
    *refs, turned = refs
    n = 2 * SIDE
    sums, outs = refs[-n:], refs[-n - ntau : -n]
    me = lax.axis_index("tau")
    order = [partner(me, shift, ntau) for shift in shifts(ntau)]
    for acc in sums:
        acc[...] = jnp.zeros_like(acc)
    work = []
    for half, (start, count) in enumerate(spans):
        near, far = refs[half * (2 * SIDE - 1) :][:SIDE], refs[half * (2 * SIDE - 1) + SIDE :][: SIDE - 1]
        for u in range(SIDE):
            rows = [far[u - 1].at[s] if u else near[s].at[0] for s in range(SIDE)]
            places = [(s, u) if half == 0 else (u, s) for s in range(SIDE)]
            bases = [(dz * SIDE + dy) * stride + start for dz, dy in places]

            work.append((rows, bases, count))
    for u in range(SIDE):
        rows, bases = work[u][0] + work[u + SIDE][0], work[u][1] + work[u + SIDE][1]

        def add(g, carry, rows=rows, bases=bases):
            for q in range(SUB):
                p = g * SUB + q
                for ref, base, acc in zip(rows, bases, sums):
                    acc[target[base + p]] += ref[p]
            return carry

        lax.fori_loop(0, work[u][2] // SUB, add, 0)

    def turn(g, carry):
        at = pl.multiple_of(g * SUB, SUB)
        total = sum([acc[pl.ds(at, SUB)] for acc in sums[1:]], sums[0][pl.ds(at, SUB)])
        turned[:, pl.ds(at, SUB), :] = jnp.swapaxes(total, 0, 1)
        return carry

    lax.fori_loop(0, sums[0].shape[0] // SUB, turn, 0)
    for r, out in zip(order, outs):
        out[...] = turned[r]


def add_tile_first(target, halves, spans, stride, ntau):
    tiles = SIDE * SIDE * CHI_DEV
    operands, specs = [], []
    for near, far in halves:
        operands += [*near, *far]
        specs += [pl.BlockSpec((1, *p.shape[1:]), lambda b, *_: (0, 0, 0, 0)) for p in near]
        specs += [pl.BlockSpec(p.shape, lambda b, *_: (0, 0, 0, 0)) for p in far]

    def kernel(*refs):
        add_tile_first_kernel(*refs, spans=spans, stride=stride, ntau=ntau)

    return pl.pallas_call(
        kernel,
        out_shape=[jax.ShapeDtypeStruct((tiles, TILE), jnp.float32)] * ntau,
        grid_spec=pltpu.PrefetchScalarGridSpec(
            num_scalar_prefetch=1,
            grid=(1,),
            in_specs=specs,
            out_specs=[pl.BlockSpec((tiles, TILE), lambda b, *_: (0, 0))] * ntau,
            scratch_shapes=[pltpu.VMEM((tiles, ntau, TILE), jnp.float32)] * (2 * SIDE)
            + [pltpu.VMEM((ntau, tiles, TILE), jnp.float32)],
        ),
        compiler_params=pltpu.CompilerParams(vmem_limit_bytes=60 * 2**20),
        name="add_tile_first",
    )(target, *operands)


def finish_kernel(target, weights, piece, *refs, start, stride, ntau, nfreq):
    times, out, sums = refs[:ntau], refs[ntau], refs[ntau + 1 :]
    step = pl.program_id(0)
    here = lax.axis_index("tau")
    origins = [partner(here, shift, ntau, back=True) for shift in shifts(ntau)]
    lower = lax.broadcasted_iota(jnp.int32, (SUB, TILE), 0) < nfreq
    me = lax.axis_index("tile")
    dz = (me // SIDE + SIDE - step) % SIDE
    bases = [(dz * SIDE + (me % SIDE + SIDE - y) % SIDE) * stride + start for y in range(SIDE)]

    @pl.when(step == 0)
    def _():
        for acc in sums:
            acc[...] = jnp.zeros_like(acc)

    def add(g, carry):
        at = pl.multiple_of(g * SUB, SUB)
        blocks = [piece[i, :, pl.ds(at, SUB), :] for i in range(SIDE)]
        pairs = [jnp.swapaxes(jnp.concatenate(blocks[i : i + 2], axis=0), 0, 1) for i in (0, 2)]
        for q in range(SUB):
            for i in range(SIDE):
                both = pairs[i // 2][q]
                mine = jnp.where(lower, 0.0, both) if i % 2 else jnp.where(lower, both, 0.0)
                sums[i][target[bases[i] + at + q]] += mine
        return carry

    lax.fori_loop(0, piece.shape[2] // SUB, add, 0)

    @pl.when(step == pl.num_programs(0) - 1)
    def _():
        scale = [[jnp.full((SUB, TILE), weights[k * ntau + t], jnp.float32) for t in origins] for k in range(nfreq)]

        def last(g, carry):
            at = pl.multiple_of(g * SUB, SUB)
            total = sum([acc[pl.ds(at, SUB)] for acc in sums[1:]], sums[0][pl.ds(at, SUB)])
            total = jnp.swapaxes(total, 0, 1)
            values = [part[pl.ds(at, SUB), :] for part in times]
            owner = g // (CHI_DEV // SUB)
            place = pl.multiple_of((g % (CHI_DEV // SUB)) * SUB, SUB)
            for k in range(nfreq):
                value = total[k] + total[k + nfreq]
                for factor, part in zip(scale[k], values):
                    value = value + factor * part
                out[owner, k, pl.ds(place, SUB), :] = value
            return carry

        lax.fori_loop(0, sums[0].shape[0] // SUB, last, 0)


def finish(target, weights, piece, start, times, stride, nfreq):
    ntau = len(times)
    tiles, width = times[0].shape
    blocks = tiles // CHI_DEV
    shape = (blocks, nfreq, CHI_DEV, width)

    def kernel(*refs):
        finish_kernel(*refs, start=start, stride=stride, ntau=ntau, nfreq=nfreq)

    return pl.pallas_call(
        kernel,
        out_shape=jax.ShapeDtypeStruct(shape, jnp.float32),
        grid_spec=pltpu.PrefetchScalarGridSpec(
            num_scalar_prefetch=2,
            grid=(blocks // SIDE,),
            in_specs=[pl.BlockSpec((SIDE, nfreq, piece.shape[2], width), lambda b, *_: (b, 0, 0, 0))]
            + [pl.BlockSpec((tiles, width), lambda b, *_: (0, 0))] * ntau,
            out_specs=pl.BlockSpec(shape, lambda b, *_: (0, 0, 0, 0)),
            scratch_shapes=[pltpu.VMEM((tiles, SUB, width), jnp.float32)] * SIDE,
        ),
        compiler_params=pltpu.CompilerParams(vmem_limit_bytes=50 * 2**20),
        name="finish",
    )(target, weights, piece, *times)


def turn_kernel(*refs):
    near, outs, held, arrived, left = refs[:SIDE], refs[SIDE:-3], *refs[-3:]
    inward = []
    for u in range(1, SIDE):
        for s in range(SIDE):
            at = (u - 1) * SIDE + s
            inward.append(pltpu.make_async_copy(near[s].at[u], held.at[u - 1, s], arrived.at[at]))
    outward = [pltpu.make_async_copy(held.at[u], out, left.at[u]) for u, out in enumerate(outs)]
    for copy in inward:
        copy.start()
    for u, copy in enumerate(outward):
        for s in range(SIDE):
            inward[u * SIDE + s].wait()
        copy.start()
    for copy in outward:
        copy.wait()


def turn(near):
    anywhere = pl.BlockSpec(memory_space=pltpu.HBM)
    return pl.pallas_call(
        turn_kernel,
        out_shape=[jax.ShapeDtypeStruct(near[0].shape, jnp.float32)] * (SIDE - 1),
        in_specs=[pl.BlockSpec(memory_space=pl.ANY)] * SIDE,
        out_specs=[anywhere] * (SIDE - 1),
        scratch_shapes=[
            pltpu.VMEM((SIDE - 1, *near[0].shape), jnp.float32),
            pltpu.SemaphoreType.DMA((SIDE * (SIDE - 1),)),
            pltpu.SemaphoreType.DMA((SIDE - 1,)),
        ],
        compiler_params=pltpu.CompilerParams(vmem_limit_bytes=60 * 2**20),
        name="turn",
    )(*near)


def over_tau(strips):
    ntau = len(strips)
    return [strips[0]] + [
        lax.ppermute(strip, "tau", [(i, partner(i, shift, ntau)) for i in range(ntau)])
        for strip, shift in zip(strips[1:], shifts(ntau)[1:])
    ]


def over_tile(rows, s, u, z_first):
    n = SIDE * SIDE
    return lax.ppermute(rows, "tile", [(i, around(i, s, u, z_first)) for i in range(n)])


def body(occupied, virtual, cos_weights, pair_occ, pair_virt, partial_target_tile):
    ntau = lax.axis_size("tau")
    blocks = lax.axis_size("tile")
    part, terms = pair_occ.shape
    nfreq = cos_weights.shape[0]
    weights = cos_weights.reshape(-1)
    occ_index = pair_occ.T
    virt_index = pair_virt.T
    slot = jnp.pad(partial_target_tile.astype(jnp.float32), (0, SUB * TILE - part)).reshape(SUB, TILE)
    stores = occupied[0], virtual[0]
    first, second = TILE_FIRST
    spans = [(0, first), (first, second)]

    near, far = [], []
    outs = list(tile_first_products(occ_index, virt_index, *stores, slot, spans, terms, blocks))
    occ_index, outs[0] = lax.optimization_barrier((occ_index, outs[0]))
    for half in range(2):
        mine, *others = outs[half * SIDE : (half + 1) * SIDE]
        near.append([mine] + [over_tile(rows, s + 1, 0, half == 0) for s, rows in enumerate(others)])
    strips = list(tau_first_products(occ_index, virt_index, *stores, first + second, TAU_FIRST, terms, ntau))
    strips = over_tau(strips)
    for half in range(2):
        far.append([over_tile(rows, 0, u + 1, half == 0) for u, rows in enumerate(turn(near[half]))])
    weighted = weigh(weights, strips, nfreq)
    piece = lax.all_to_all(weighted, "tile", 0, 0, tiled=True)

    lines = -(-part // TILE)
    stride = lines * TILE
    by_u = [jnp.stack([n[0, first, :lines] for n in near[0]])] + [f[:, first, :lines] for f in far[0]]
    target = jnp.stack(by_u, axis=1).astype(jnp.int32).reshape(-1)
    chi = add_tile_first(target, list(zip(near, far)), spans, stride, ntau)
    times = over_tau(chi)
    spectrum = finish(target, weights, piece, first + second, times, stride, nfreq)
    owned = lax.all_to_all(spectrum, "tile", 0, 0, tiled=True)
    return jnp.transpose(owned, (1, 2, 0, 3))


def solution(mesh):
    in_specs = (
        P("tau", "tile", None, None),
        P("tau", "tile", None, None),
        P(),
        P("tile", None),
        P("tile", None),
        P("tile"),
    )
    out_specs = P(None, "tile", "tau", None)

    return jax.shard_map(body, mesh=mesh, in_specs=in_specs, out_specs=out_specs, check_vma=False)
```
